32 devices in a mesh: grp: 4 (over z), hap: 8 (over y, x, core).
Axes of the slice: x: 2, y: 2, z: 4, core: 2. Of those that a mesh axis runs over, the one named last changes fastest.
Arguments:
- alleles: int32 [60, 512], P('grp', 'hap'), may hold values from 0 to 1073741823
- observed: int32 [60, 32], P('grp', 'hap'), may hold values from 0 to 2
- map_steps: int32 [60], P('grp'), may hold values from 1 to 99
- start_weights: float32 [32, 15360], P('hap'), may hold values from 1e-12 to 1
- end_weights: float32 [32, 15360], P('hap'), may hold values from 1e-12 to 1
Outputs:
- dosage: float32 [60, 32], P('grp', 'hap')
The draws below stay inside these ranges and needn't reach their ends.
Inputs may be any that keep to these rules, and one draw needn't show every extreme that they name: Bit b of alleles[m, w] is the allele 0 or 1 of reference haplotype 30 w + b at marker m. 0 and 1 are observed alleles, 2 marks a marker not typed in that target.
All inputs are finite; a program needn't handle non-finite values.
Results may differ from the reference program's by a relative error of at most 0.0008.
Values sent between devices are 32-bit elements; how exact they have to be, the bound alone decides.
A program may use at most 128 MiB of HBM per device.

```python
import math
import jax
import jax.numpy as jnp
from jax import lax

K = 15360
TGT_DEV = 4
WORDS = 512
MARKERS = 60
TARGETS = 32


def place_ends(entries, own_key, smallest, top_value):
    spot = [jax.random.randint(jax.random.fold_in(own_key, axis), (), 0, length) for axis, length in enumerate(entries.shape)]
    longest = entries.shape.index(max(entries.shape))
    next_to = spot[:longest] + [(spot[longest] + 1) % entries.shape[longest]] + spot[longest + 1:]
    return entries.at[tuple(spot)].set(smallest).at[tuple(next_to)].set(top_value)


def block_levels(rng, extent, pieces, smallest, top_value):
    level = 1.0
    for axis_at, parts in pieces:
        heights = jax.random.uniform(jax.random.fold_in(jax.random.fold_in(rng, 6), axis_at), (parts,), jnp.float32, smallest / len(pieces), top_value / len(pieces))
        level = level * jnp.repeat(jnp.exp(heights), extent[axis_at] // parts).reshape((-1,) + (1,) * (len(extent) - 1 - axis_at))
    return level


def setup_inputs(seed: int = 0) -> dict:
    key_of = jax.random.split(jax.random.key(seed), 6)
    return {
        "alleles": place_ends(jax.random.randint(key_of[0], (MARKERS, WORDS), 0, 1073741824), jax.random.fold_in(key_of[0], 1), 0, 1073741823).astype(jnp.int32),
        "observed": place_ends(jax.random.randint(key_of[1], (MARKERS, TARGETS), 0, 3), jax.random.fold_in(key_of[1], 1), 0, 2).astype(jnp.int32),
        "map_steps": place_ends(jax.random.randint(key_of[2], (MARKERS,), 1, 100), jax.random.fold_in(key_of[2], 1), 1, 99).astype(jnp.int32),
        "start_weights": jnp.clip(jnp.exp(math.log(1.0) - 27.631021 * jax.random.uniform(key_of[3], (TARGETS, K), jnp.float32) ** block_levels(key_of[3], (TARGETS, K), ((0, 8),), -0.2, 0.2)), 9.999999960041972e-13, 1.0),
        "end_weights": jnp.clip(jnp.exp(math.log(1.0) - 27.631021 * jax.random.uniform(key_of[4], (TARGETS, K), jnp.float32) ** block_levels(key_of[4], (TARGETS, K), ((0, 8),), -0.2, 0.2)), 9.999999960041972e-13, 1.0),
    }


error_rate = 0.01
map_unit = 100000.0


def unpack_alleles(packed):
    shifts = jnp.arange(30, dtype=jnp.int32)
    bits = jnp.bitwise_and(jnp.right_shift(packed[:, :, None], shifts[None, None, :]), 1)
    return bits.reshape(packed.shape[0], packed.shape[1] * 30).astype(jnp.float32)


def emission(allele_row, observed_col):
    missing = (observed_col == 2).astype(jnp.float32)[:, None]
    called = observed_col.astype(jnp.float32)[:, None]
    agree = allele_row[None, :] * called + (1.0 - allele_row[None, :]) * (1.0 - called)
    return missing + (1.0 - missing) * (error_rate + (1.0 - 2.0 * error_rate) * agree)


def forward_pass(state, haplos, observed, rates):
    total_haps = haplos.shape[1]

    def advance(carry, inputs):
        allele_row, observed_col, rate = inputs
        mixed = (1.0 - rate) * carry + (rate / total_haps) * jnp.sum(carry, axis=1, keepdims=True)
        weighted = emission(allele_row, observed_col) * mixed
        weighted = weighted / jnp.sum(weighted, axis=1, keepdims=True)
        return weighted, weighted.astype(jnp.bfloat16)

    return lax.scan(advance, state, (haplos, observed, rates))


def backward_pass(state, haplos, observed, rates):
    total_haps = haplos.shape[1]

    def retreat(carry, inputs):
        allele_row, observed_col, rate = inputs
        kept = carry.astype(jnp.bfloat16)
        weighted = emission(allele_row, observed_col) * carry
        mixed = (1.0 - rate) * weighted + (rate / total_haps) * jnp.sum(weighted, axis=1, keepdims=True)
        mixed = mixed / jnp.sum(mixed, axis=1, keepdims=True)
        return mixed, kept

    return lax.scan(retreat, state, (haplos, observed, rates), reverse=True)


def reference(alleles, observed, map_steps, start_weights, end_weights):
    haplos = unpack_alleles(alleles)
    rates = 1.0 - jnp.exp(-map_steps.astype(jnp.float32) / map_unit)
    start_rows = start_weights / jnp.sum(start_weights, axis=1, keepdims=True)
    end_rows = end_weights / jnp.sum(end_weights, axis=1, keepdims=True)
    blocks = TARGETS // TGT_DEV
    observed_blocks = observed.reshape(MARKERS, blocks, TGT_DEV).transpose(1, 0, 2)
    start_blocks = start_rows.reshape(blocks, TGT_DEV, K)
    end_blocks = end_rows.reshape(blocks, TGT_DEV, K)
    allele_half = haplos.astype(jnp.bfloat16)

    def one_block(operands):
        observed_block, start_block, end_block = operands
        _, forward_store = forward_pass(start_block, haplos, observed_block, rates)
        _, backward_store = backward_pass(end_block, haplos, observed_block, rates)
        forward_store = lax.optimization_barrier(forward_store)
        backward_store = lax.optimization_barrier(backward_store)
        carrying = backward_store * allele_half[:, None, :]
        forward_wide = forward_store.astype(jnp.float32)
        numer = jnp.einsum("mtk,mtk->mt", forward_wide, carrying.astype(jnp.float32))
        denom = jnp.einsum("mtk,mtk->mt", forward_wide, backward_store.astype(jnp.float32))
        return numer / denom

    dosage = lax.map(one_block, (observed_blocks, start_blocks, end_blocks))
    return dosage.transpose(1, 0, 2).reshape(MARKERS, TARGETS)
```

```python
import functools
import jax
import jax.numpy as jnp
from jax import lax
from jax.experimental import pallas as pl
from jax.experimental.pallas import tpu as pltpu
from jax.sharding import PartitionSpec as P

error_rate = 0.01
map_unit = 100000.0
SUB, LANE = 8, 128
MESH = pl.DeviceIdType.MESH


def total(parts):
    parts = list(parts)
    while len(parts) > 1:
        parts = [a + b for a, b in zip(parts[::2], parts[1::2])] + parts[len(parts) // 2 * 2:]
    return parts[0]


def block_size(local_m):
    return next(n for n in (5, 4, 3, 2, 1) if local_m % n == 0)


def kernel(dims, alleles, observed, steps, starts, ends, out,
           own_alleles, own_observed, own_steps, tmp, col, recv, bits, table, weights, staged,
           state_a, state_b, emit, runs, kept, kept_low, waiting, numer, denom, dos, out_recv,
           load_sem, z_send, z_recv, p_send, p_recv, out_send, out_recv_sem):
    groups, haps, local_m, targets, words, bits_word = dims
    total_haps = words * bits_word
    local_w = words // haps
    span = words // SUB
    reps = LANE // span
    vecs = bits_word // reps
    pack = LANE // local_w
    rows = -(-local_m // pack)
    slots = pack * rows
    share = haps // SUB
    half = groups // 2
    size = block_size(local_m)
    blocks = local_m // size
    end_row = groups * slots
    g_me, h_me = lax.axis_index("grp"), lax.axis_index("hap")
    mine = lax.rem(g_me, targets)
    near = g_me < half

    loads = [
        pltpu.make_async_copy(source, target, load_sem.at[n]) for n, (source, target) in enumerate([
            (alleles, own_alleles), (observed, own_observed), (steps, own_steps),
            (starts, weights.at[0]), (ends, weights.at[1])])
    ]
    for load in loads:
        load.start()

    def each_hap(act):
        if haps <= 8:
            for d in range(1, haps):
                act(lax.rem(h_me + d, haps))
        else:
            pl.loop(1, haps)(lambda d: act(lax.rem(h_me + d, haps)))

    def each_group_step(act):
        if groups <= 4:
            for d in range(1, groups):
                act(d)
        else:
            pl.loop(1, groups)(act)

    barrier = pltpu.get_barrier_semaphore()

    def greet(g, h):
        pl.semaphore_signal(barrier, inc=1, device_id=(g, h), device_id_type=MESH)

    pl.when(g_me > 0)(lambda: greet(g_me - 1, h_me))
    each_group_step(lambda d: pl.when(g_me + d < groups)(lambda: greet(g_me + d, h_me)))
    each_hap(lambda h: greet(g_me, h))

    lane = lax.broadcasted_iota(jnp.int32, (SUB, LANE), 1)
    sub_at = lax.broadcasted_iota(jnp.int32, (SUB, LANE), 0)
    tmp[...] = jnp.zeros_like(tmp)
    for load in loads[:3]:
        load.wait()
    tmp[0:local_m, 0:local_w] = own_alleles[...]
    dense = tmp[0:SUB, :]
    for p in range(1, pack):
        dense = jnp.where(lane // local_w == p, pltpu.roll(tmp[p * rows:p * rows + SUB, :], p * local_w, 1), dense)
    col[g_me, 0:SUB, :] = dense
    recv[g_me, pl.ds(pl.multiple_of(h_me * SUB, SUB), SUB), :] = dense
    tmp[0:targets, 0:local_m] = own_observed[...]
    columns = tmp[0:SUB, :]
    for i in range(local_m):
        columns = jnp.where((sub_at == targets) & (lane == i), own_steps[i], columns)
    col[g_me, SUB:2 * SUB, :] = columns

    def z_copy(block, g):
        return pltpu.make_async_remote_copy(
            src_ref=col.at[block], dst_ref=col.at[block], send_sem=z_send.at[block, g], recv_sem=z_recv.at[block],
            device_id=(g, h_me), device_id_type=MESH)

    def p_copy(block, h, sem_h):
        return pltpu.make_async_remote_copy(
            src_ref=col.at[block, 0:SUB], dst_ref=recv.at[block, pl.ds(pl.multiple_of(sem_h * SUB, SUB), SUB), :],
            send_sem=p_send.at[block, h], recv_sem=p_recv.at[block, sem_h],
            device_id=(g_me, h), device_id_type=MESH)

    def spread(block):
        each_hap(lambda h: p_copy(block, h, h_me).start())

    def each_z_copy(act):
        pl.when(g_me + 1 < groups)(lambda: act(z_copy(g_me, g_me + 1)))
        each_group_step(lambda d: pl.when(g_me - d >= 0)(lambda: act(z_copy(g_me, g_me - d))))

    pl.semaphore_wait(barrier, g_me + jnp.where(g_me < groups - 1, 1, 0) + haps - 1)
    each_z_copy(lambda copy: copy.start())
    spread(g_me)

    def arrange(which, state):
        source_rows = weights.at[which]
        for r in range(vecs):
            for s in range(SUB):
                at = s * vecs + r
                staged[at * targets:(at + 1) * targets, :] = source_rows[:, at * LANE:(at + 1) * LANE]
        source = [staged[pl.ds(r * targets + mine, SUB, stride=vecs * targets), :] for r in range(vecs)]
        result = []
        for q in range(vecs):
            spot = bits_word * (lane % span) + reps * q + lane // span
            chosen, within = spot // LANE, spot % LANE
            value = jnp.zeros((SUB, LANE), jnp.float32)
            for r in range(vecs):
                moved = jnp.take_along_axis(source[r], within, axis=1, mode="promise_in_bounds")
                value = jnp.where(chosen == r, moved, value)
            state[q] = value
            result.append(value)
        return 1.0 / add_up(total(result))

    def add_up(value):
        for shift in (4, 2, 1):
            value = value + pltpu.roll(value, shift, 0)
        return jnp.broadcast_to(jnp.sum(value, axis=1, keepdims=True), (SUB, LANE))

    for load in loads[3:]:
        load.wait()
    scale_a = arrange(jnp.where(near, 0, 1), state_a)

    def arrived(block):
        z_copy(block, g_me).wait_recv()

    def keep_own(block):
        recv[block, pl.ds(pl.multiple_of(h_me * SUB, SUB), SUB), :] = col[block, 0:SUB, :]

    def relay(d):
        low, high = g_me - d, g_me + d

        @pl.when(low >= 0)
        def _():
            arrived(low)
            pl.when(g_me + 1 < groups)(z_copy(low, g_me + 1).start)
            spread(low)
            keep_own(low)

        @pl.when(high < groups)
        def _():
            arrived(high)
            spread(high)
            keep_own(high)

    if groups <= 4:
        relay(1)
        scale_b = arrange(jnp.where(near, 1, 0), state_b)
        for d in range(2, groups):
            relay(d)
    else:
        scale_b = arrange(jnp.where(near, 1, 0), state_b)
        pl.loop(1, groups)(relay)

    table[2, end_row:end_row + SUB, :] = jnp.zeros((SUB, LANE), jnp.float32)

    @pl.loop(0, groups)
    def _(g):
        same = lax.broadcasted_iota(jnp.int32, (slots, LANE), 0) == lax.broadcasted_iota(jnp.int32, (slots, LANE), 1)

        def turned(at):
            values = jnp.broadcast_to(col[g, pl.ds(SUB + at, 1), :].astype(jnp.float32), (slots, LANE))
            summed = jnp.sum(jnp.where(same, values, 0.0), axis=1, keepdims=True)
            return jnp.broadcast_to(summed, (slots, LANE))

        seen, dist = turned(mine), turned(targets)
        rate = 1.0 - jnp.exp(-dist / map_unit)
        at = pl.ds(pl.multiple_of(g * slots, SUB), slots)
        table[0, at, :] = jnp.where(seen == 2.0, 1.0, jnp.where(seen == 1.0, 1.0 - error_rate, error_rate))
        table[1, at, :] = jnp.where(seen == 2.0, 1.0, jnp.where(seen == 0.0, 1.0 - error_rate, error_rate))
        table[2, at, :] = (rate / total_haps) / (1.0 - rate)

    def group_at(s):
        return jnp.where(near, s, groups - 1 - s)

    def marker_at(n):
        return jnp.where(near, n, local_m - 1 - n)

    def expand(s):
        g = group_at(s)
        each_hap(lambda h: p_copy(g, h, h).wait_recv())
        for r in range(rows):
            parts = [recv[g, pl.ds(j * SUB + r, SUB, stride=SUB * share), :] for j in range(share)]
            for p in range(pack):
                n = p * rows + r
                if n >= local_m:
                    continue
                value = jnp.zeros((SUB, LANE), jnp.int32)
                for e in range(reps):
                    for j in range(share):
                        begin = e * span + j * local_w
                        shift = (begin - p * local_w) % LANE
                        piece = parts[j] if shift == 0 else pltpu.roll(parts[j], shift, 1)
                        piece = piece if e == 0 else jnp.right_shift(piece, e)
                        value = jnp.where((lane >= begin) & (lane < begin + local_w), piece, value)
                bits[s * slots + marker_at(n)] = value

    def row(kind, slot):
        return jnp.broadcast_to(table[kind, pl.ds(slot, 1), :], (SUB, LANE))

    def share_rows(s, n):
        g, at = group_at(s), marker_at(n)
        this = g * slots + at
        after = jnp.where(at + 1 < local_m, this + 1, jnp.where(g + 1 < groups, (g + 1) * slots, end_row))
        return jnp.where(near, this, after), jnp.where(near, after, this)

    def masked(words_in, q):
        return jnp.bitwise_and(words_in, 1 << (reps * q)) != 0

    pairs = [(j, i) for j in range(size) for i in range(j, size)]

    def prepare(s, n):
        at = s * slots + n * size
        sums = {}
        words_in = [bits[at + i] for i in range(size)]
        tops = []
        for i in range(size):
            slot = group_at(s) * slots + marker_at(n * size + i)
            tops.append((row(0, slot), row(1, slot)))
        for q in range(vecs):
            e = [jnp.where(masked(words_in[i], q), *tops[i]) for i in range(size)]
            for i in range(size):
                emit[at + i, q] = e[i]
            for j in range(size):
                run = e[j]
                for i in range(j, size):
                    run = run if i == j else run * e[i]
                    sums[j, i] = run if q == 0 else sums[j, i] + run
        for k, pair in enumerate(pairs):
            runs[s * blocks + n, k] = add_up(sums[pair])

    def solve(state, scale, s, n, order, which):
        at = s * slots + n * size
        sums = [None] * size
        for q in range(vecs):
            value = state[q]
            for i in order:
                value = value * emit[at + i, q]
                sums[i] = value if q == 0 else sums[i] + value
        span_of = {pair: runs[s * blocks + n, k] for k, pair in enumerate(pairs)}
        adds = {}
        last = None
        for i in order:
            share_of = row(2, share_rows(s, n * size + i)[which])
            adds[i] = share_of if last is None else share_of * last
            last = add_up(sums[i]) * scale
            for j in adds:
                last = last + adds[j] * span_of[min(i, j), max(i, j)]
        return adds, 1.0 / last

    up, down = list(range(size)), list(range(size))[::-1]

    def step_a(s, n, scale):
        at = s * slots + n * size
        adds, after = solve(state_a, scale, s, n, up, 0)
        words_in = [bits[at + i] for i in range(size)]
        for q in range(vecs):
            value = state_a[q] * scale
            for i in up:
                value = emit[at + i, q] * (value + adds[i])
                kept[at + i, q] = jnp.where(masked(words_in[i], q), value, 0.0)
            kept_low[s * blocks + n, q] = value
            state_a[q] = value
        return after

    def put_sums(s, n, tops, low):
        for i in range(size):
            at = pl.ds(pl.multiple_of((s * slots + n * size + i) * SUB, SUB), SUB)
            numer[at, :] = tops[i]
            denom[at, :] = low

    def step_b(s, n, scale, score):
        at = s * slots + n * size
        adds, after = solve(state_b, scale, s, n, down, 1)
        tops, low = [None] * size, None
        for q in range(vecs):
            value = state_b[q] * scale
            for i in down:
                value = value + adds[i]
                if score:
                    part = kept[at + i, q] * value
                    tops[i] = part if q == 0 else tops[i] + part
                    if i == size - 1:
                        part = kept_low[s * blocks + n, q] * value
                        low = part if q == 0 else low + part
                else:
                    waiting[n * size + i, q] = value
                value = emit[at + i, q] * value
            state_b[q] = value
        if score:
            put_sums(s, n, tops, low)
        return after

    def score_waiting(s, n):
        at = s * slots + n * size
        tops = [total(kept[at + i, q] * waiting[n * size + i, q] for q in range(vecs)) for i in range(size)]
        last = n * size + size - 1
        put_sums(s, n, tops, total(kept_low[s * blocks + n, q] * waiting[last, q] for q in range(vecs)))

    owner = g_me < targets

    def out_copy(g, target):
        return pltpu.make_async_remote_copy(
            src_ref=dos.at[g], dst_ref=out_recv.at[target], send_sem=out_send.at[g],
            recv_sem=out_recv_sem.at[target], device_id=(g, h_me), device_id_type=MESH)

    row_at = lax.broadcasted_iota(jnp.int32, (slots, LANE), 0)
    own_lane = lax.broadcasted_iota(jnp.int32, (slots, LANE), 1) == jnp.where(near, row_at, local_m - 1 - row_at)

    def finish(s):
        g = group_at(s)

        def gathered(sums):
            parts = [sums[pl.ds(s * slots * SUB + k, slots, stride=SUB), :] for k in range(SUB)]
            return jnp.sum(total(parts), axis=1, keepdims=True)

        value = jnp.broadcast_to(gathered(numer) / gathered(denom), (slots, LANE))
        value = jnp.where(own_lane & (row_at < local_m), value, 0.0)
        dos[g] = jnp.broadcast_to(jnp.sum(value, axis=0, keepdims=True), (SUB, LANE))
        pl.when((g != g_me) & owner)(lambda: out_copy(g, g_me).start())

    def first_pass(s, scale):
        expand(s)
        for n in range(blocks):
            prepare(s, n)
            scale = step_a(s, n, scale)
        return scale

    far = groups - 1
    scale_a = lax.fori_loop(0, far, first_pass, scale_a)
    expand(far)
    ready = set()
    for n in range(blocks):
        for k in (n, blocks - 1 - n):
            if k not in ready:
                ready.add(k)
                prepare(far, k)
        scale_a = step_a(far, n, scale_a)
        scale_b = step_b(far, blocks - 1 - n, scale_b, False)
    for n in range(blocks):
        score_waiting(far, n)

    def second_pass(k, scale):
        s = far - 1 - k
        finish(s + 1)
        for n in reversed(range(blocks)):
            scale = step_b(s, n, scale, True)
        return scale

    lax.fori_loop(0, far, second_pass, scale_b)
    finish(0)

    each_z_copy(lambda copy: copy.wait_send())
    each_hap(lambda h: p_copy(g_me, h, h_me).wait_send())

    def drain(d):
        low, high = g_me - d, g_me + d

        @pl.when(low >= 0)
        def _():
            pl.when(g_me + 1 < groups)(lambda: z_copy(low, g_me + 1).wait_send())
            each_hap(lambda h: p_copy(low, h, h_me).wait_send())

        @pl.when(high < groups)
        def _():
            each_hap(lambda h: p_copy(high, h, h_me).wait_send())

    each_group_step(drain)

    @pl.when(owner)
    def _():
        out_recv[g_me] = dos[g_me]
        each_group_step(lambda d: out_copy(lax.rem(g_me + d, groups), g_me).wait_send())

    @pl.loop(0, targets)
    def _(t):
        pl.when(t != g_me)(lambda: out_copy(g_me, t).wait_recv())

    result = out_recv[0]
    for t in range(1, targets):
        result = jnp.where(sub_at == t, out_recv[t], result)
    out[...] = result[0:targets, 0:local_m]


def solution(mesh):
    groups, haps = mesh.shape["grp"], mesh.shape["hap"]

    def local(alleles, observed, map_steps, start_weights, end_weights):
        local_m, local_w = alleles.shape
        targets, total_haps = start_weights.shape
        words = local_w * haps
        bits_word = total_haps // words
        reps = LANE * SUB // words
        vecs = bits_word // reps
        pack = LANE // local_w
        slots = pack * -(-local_m // pack)
        size = block_size(local_m)
        blocks = groups * (local_m // size)
        assert targets < SUB and targets <= groups and groups % 2 == 0 and slots % SUB == 0
        dims = (groups, haps, local_m, targets, words, bits_word)
        f32, i32 = jnp.float32, jnp.int32
        dma = pltpu.SemaphoreType.DMA
        tile = (SUB, LANE)
        out = pl.pallas_call(
            functools.partial(kernel, dims),
            out_shape=jax.ShapeDtypeStruct((targets, local_m), f32),
            in_specs=[pl.BlockSpec(memory_space=pltpu.HBM)] * 5,
            out_specs=pl.BlockSpec(memory_space=pltpu.VMEM),
            scratch_shapes=[
                pltpu.VMEM((local_m, local_w), i32),
                pltpu.VMEM((targets, local_m), i32),
                pltpu.SMEM((local_m,), i32),
                pltpu.VMEM((slots + SUB, LANE), i32),
                pltpu.VMEM((groups, 2 * SUB, LANE), i32),
                pltpu.VMEM((groups, haps * SUB, LANE), i32),
                pltpu.VMEM((groups * slots, *tile), i32),
                pltpu.VMEM((3, groups * slots + SUB, LANE), f32),
                pltpu.VMEM((2, targets, total_haps), f32),
                pltpu.VMEM((vecs * SUB * targets, LANE), f32),
                pltpu.VMEM((vecs, *tile), f32),
                pltpu.VMEM((vecs, *tile), f32),
                pltpu.VMEM((groups * slots, vecs, *tile), f32),
                pltpu.VMEM((blocks, size * (size + 1) // 2, *tile), f32),
                pltpu.VMEM((groups * slots, vecs, *tile), f32),
                pltpu.VMEM((blocks, vecs, *tile), f32),
                pltpu.VMEM((local_m, vecs, *tile), f32),
                pltpu.VMEM((groups * slots * SUB, LANE), f32),
                pltpu.VMEM((groups * slots * SUB, LANE), f32),
                pltpu.VMEM((groups, *tile), f32),
                pltpu.VMEM((targets, *tile), f32),
                dma((5,)), dma((groups, groups)), dma((groups,)), dma((groups, haps)), dma((groups, haps)),
                dma((groups,)), dma((targets,)),
            ],
            compiler_params=pltpu.CompilerParams(
                collective_id=0, has_side_effects=True, vmem_limit_bytes=60 * 1024 * 1024),
        )(alleles, observed.T, map_steps, start_weights, end_weights)
        return out.T

    in_specs = (P("grp", "hap"), P("grp", "hap"), P("grp"), P("hap", None), P("hap", None))
    return jax.shard_map(local, mesh=mesh, in_specs=in_specs, out_specs=P("grp", "hap"), check_vma=False)
```

```python
import functools
import jax
import jax.numpy as jnp
from jax import lax
from jax.experimental import pallas as pl
from jax.experimental.pallas import tpu as pltpu
from jax.sharding import PartitionSpec as P

error_rate = 0.01
map_unit = 100000.0
SUB, LANE = 8, 128
MESH = pl.DeviceIdType.MESH


def total(parts):
    parts = list(parts)
    while len(parts) > 1:
        parts = [a + b for a, b in zip(parts[::2], parts[1::2])] + parts[len(parts) // 2 * 2:]
    return parts[0]


def block_size(local_m):
    return next(n for n in (5, 4, 3, 2, 1) if local_m % n == 0)


def targets_each(targets, state_bytes):
    return 2 if targets % 2 == 0 and 4 * state_bytes <= 40 * 1024 * 1024 else 1


def kernel(dims, alleles, observed, steps, starts, ends, out,
           own_alleles, own_observed, own_steps, tmp, block, meta, recv, metas, bits, table, weights, staged,
           state_a, state_b, emit, runs, kept, kept_low, waiting, numer, denom, dos, out_recv,
           load_sem, send_sem, recv_sem, meta_send, meta_recv, out_send, out_recv_sem):
    groups, haps, local_m, targets, words, bits_word = dims
    total_haps = words * bits_word
    local_w = words // haps
    span = words // SUB
    reps = LANE // span
    vecs = bits_word // reps
    pack = LANE // local_w
    rows = -(-local_m // pack)
    slots = pack * rows
    share = haps // SUB
    size = block_size(local_m)
    blocks = local_m // size
    end_row = groups * slots
    each = targets_each(targets, groups * slots * total_haps * 4)
    teams = targets // each
    far = groups - 1
    g_me, h_me = lax.axis_index("grp"), lax.axis_index("hap")
    active = g_me < teams

    sources = [
        (alleles, own_alleles), (observed, own_observed), (steps, own_steps), (starts, weights.at[0]), (ends, weights.at[1])]
    loads = [pltpu.make_async_copy(source, target, load_sem.at[n]) for n, (source, target) in enumerate(sources)]
    for load in loads[:3]:
        load.start()

    def each_hap(act, first=0):
        if haps <= 8:
            for d in range(first, haps):
                act(lax.rem(h_me + d, haps))
        else:
            pl.loop(first, haps)(lambda d: act(lax.rem(h_me + d, haps)))

    def each_group(act):
        if groups <= 4:
            for g in reversed(range(groups)):
                act(g)
        else:
            pl.loop(0, groups)(lambda k: act(far - k))

    def not_me(g, h, act):
        pl.when((g != g_me) | (h != h_me))(act)

    barrier = pltpu.get_barrier_semaphore()

    def greet(g, h):
        pl.semaphore_signal(barrier, inc=1, device_id=(g, h), device_id_type=MESH)

    @pl.when(active)
    def _():
        each_group(lambda g: each_hap(lambda h: not_me(g, h, lambda: greet(g, h))))
        for load in loads[3:]:
            load.start()

    lane = lax.broadcasted_iota(jnp.int32, (SUB, LANE), 1)
    sub_at = lax.broadcasted_iota(jnp.int32, (SUB, LANE), 0)
    tmp[...] = jnp.zeros_like(tmp)
    for load in loads[:3]:
        load.wait()
    tmp[0:local_m, 0:local_w] = own_alleles[...]
    dense = tmp[0:SUB, :]
    for p in range(1, pack):
        dense = jnp.where(lane // local_w == p, pltpu.roll(tmp[p * rows:p * rows + SUB, :], p * local_w, 1), dense)
    block[...] = dense
    recv[g_me, pl.ds(pl.multiple_of(h_me * SUB, SUB), SUB), :] = dense
    tmp[0:targets, 0:local_m] = own_observed[...]
    columns = tmp[0:SUB, :]
    for i in range(local_m):
        columns = jnp.where((sub_at == targets) & (lane == i), own_steps[i], columns)
    meta[...] = columns
    metas[g_me] = columns

    def block_copy(g, h, from_g, from_h):
        return pltpu.make_async_remote_copy(
            src_ref=block, dst_ref=recv.at[from_g, pl.ds(pl.multiple_of(from_h * SUB, SUB), SUB), :],
            send_sem=send_sem.at[g, h], recv_sem=recv_sem.at[from_g, from_h],
            device_id=(g, h), device_id_type=MESH)

    def meta_copy(g, from_g):
        return pltpu.make_async_remote_copy(
            src_ref=meta, dst_ref=metas.at[from_g], send_sem=meta_send.at[g], recv_sem=meta_recv.at[from_g],
            device_id=(g, h_me), device_id_type=MESH)

    def each_send(act):
        for g in range(teams):
            pl.when(g != g_me)(lambda: act(meta_copy(g, g_me)))
            each_hap(lambda h: not_me(g, h, lambda: act(block_copy(g, h, g_me, h_me))))

    pl.semaphore_wait(barrier, teams * haps - jnp.where(active, 1, 0))
    each_send(lambda copy: copy.start())

    def add_up(value):
        for shift in (4, 2, 1):
            value = value + pltpu.roll(value, shift, 0)
        return jnp.broadcast_to(jnp.sum(value, axis=1, keepdims=True), (SUB, LANE))

    def arrange(which, state):
        for r in range(vecs):
            for s in range(SUB):
                at = s * vecs + r
                staged[at * targets:(at + 1) * targets, :] = weights[which, :, at * LANE:(at + 1) * LANE]
        first = g_me * each
        sums = [None] * each
        for q in range(vecs):
            spot = bits_word * (lane % span) + reps * q + lane // span
            chosen, within = spot // LANE, spot % LANE
            value = [jnp.zeros((SUB, LANE), jnp.float32)] * each
            for r in range(vecs):
                here = chosen == r
                for t in range(each):
                    source = staged[pl.ds(r * targets + first + t, SUB, stride=vecs * targets), :]
                    moved = jnp.take_along_axis(source, within, axis=1, mode="promise_in_bounds")
                    value[t] = jnp.where(here, moved, value[t])
            for t in range(each):
                state[t, q] = value[t]
                sums[t] = value[t] if q == 0 else sums[t] + value[t]
        return tuple(1.0 / add_up(sums[t]) for t in range(each))

    def read_meta(g):
        pl.when(g != g_me)(lambda: meta_copy(g_me, g).wait_recv())
        same = lax.broadcasted_iota(jnp.int32, (slots, LANE), 0) == lax.broadcasted_iota(jnp.int32, (slots, LANE), 1)

        def turned(at):
            values = jnp.broadcast_to(metas[g, pl.ds(at, 1), :].astype(jnp.float32), (slots, LANE))
            summed = jnp.sum(jnp.where(same, values, 0.0), axis=1, keepdims=True)
            return jnp.broadcast_to(summed, (slots, LANE))

        at = pl.ds(pl.multiple_of(g * slots, SUB), slots)
        for t in range(each):
            seen = turned(g_me * each + t)
            table[2 * t, at, :] = jnp.where(seen == 2.0, 1.0, jnp.where(seen == 1.0, 1.0 - error_rate, error_rate))
            table[2 * t + 1, at, :] = jnp.where(seen == 2.0, 1.0, jnp.where(seen == 0.0, 1.0 - error_rate, error_rate))
        rate = 1.0 - jnp.exp(-turned(targets) / map_unit)
        table[2 * each, at, :] = (rate / total_haps) / (1.0 - rate)

    def expand(g):
        each_hap(lambda h: not_me(g, h, lambda: block_copy(g_me, h_me, g, h).wait_recv()))
        for r in range(rows):
            parts = [recv[g, pl.ds(j * SUB + r, SUB, stride=SUB * share), :] for j in range(share)]
            for p in range(pack):
                n = p * rows + r
                if n >= local_m:
                    continue
                value = jnp.zeros((SUB, LANE), jnp.int32)
                for e in range(reps):
                    for j in range(share):
                        begin = e * span + j * local_w
                        shift = (begin - p * local_w) % LANE
                        piece = parts[j] if shift == 0 else pltpu.roll(parts[j], shift, 1)
                        piece = piece if e == 0 else jnp.right_shift(piece, e)
                        value = jnp.where((lane >= begin) & (lane < begin + local_w), piece, value)
                bits[g * slots + n] = value

    def row(kind, slot):
        return jnp.broadcast_to(table[kind, pl.ds(slot, 1), :], (SUB, LANE))

    def masked(words_in, q):
        return jnp.bitwise_and(words_in, 1 << (reps * q)) != 0

    pairs = [(j, i) for j in range(size) for i in range(j, size)]
    team = range(each)

    def prepare(g, n):
        at = g * slots + n * size
        sums = {}
        words_in = [bits[at + i] for i in range(size)]
        tops = [[(row(2 * t, at + i), row(2 * t + 1, at + i)) for i in range(size)] for t in team]
        for q in range(vecs):
            masks = [masked(words_in[i], q) for i in range(size)]
            for t in team:
                e = [jnp.where(masks[i], *tops[t][i]) for i in range(size)]
                for i in range(size):
                    emit[t, at + i, q] = e[i]
                for j in range(size):
                    run = e[j]
                    for i in range(j, size):
                        run = run if i == j else run * e[i]
                        sums[t, j, i] = run if q == 0 else sums[t, j, i] + run
        for t in team:
            for k, (j, i) in enumerate(pairs):
                runs[t, g * blocks + n, k] = add_up(sums[t, j, i])

    def solve(t, state, scale, g, n, order, after):
        at = g * slots + n * size
        sums = [None] * size
        for q in range(vecs):
            value = state[t, q]
            for i in order:
                value = value * emit[t, at + i, q]
                sums[i] = value if q == 0 else sums[i] + value
        span_of = {pair: runs[t, g * blocks + n, k] for k, pair in enumerate(pairs)}
        adds = {}
        last = None
        for i in order:
            slot = at + i
            if after:
                slot = slot + 1
                if i == size - 1:
                    ahead = jnp.where(g + 1 < groups, (g + 1) * slots, end_row)
                    slot = jnp.where(n * size + size == local_m, ahead, slot)
            adds[i] = row(2 * each, slot) if last is None else row(2 * each, slot) * last
            last = add_up(sums[i]) * scale
            for j in adds:
                last = last + adds[j] * span_of[min(i, j), max(i, j)]
        return adds, 1.0 / last

    up, down = list(range(size)), list(range(size))[::-1]

    def step_a(g, n, scale):
        at = g * slots + n * size
        solved = [solve(t, state_a, scale[t], g, n, up, False) for t in team]
        words_in = [bits[at + i] for i in range(size)]
        for q in range(vecs):
            masks = [masked(words_in[i], q) for i in range(size)]
            for t in team:
                value = state_a[t, q] * scale[t]
                for i in up:
                    value = emit[t, at + i, q] * (value + solved[t][0][i])
                    kept[t, at + i, q] = jnp.where(masks[i], value, 0.0)
                kept_low[t, g * blocks + n, q] = value
                state_a[t, q] = value
        return tuple(solved[t][1] for t in team)

    def put_sums(t, g, n, tops, low):
        for i in range(size):
            at = pl.ds(pl.multiple_of((g * slots + n * size + i) * SUB, SUB), SUB)
            numer[t, at, :] = tops[i]
            denom[t, at, :] = low

    def step_b(g, n, scale, score):
        at = g * slots + n * size
        result = []
        for t in team:
            adds, after = solve(t, state_b, scale[t], g, n, down, True)
            result.append(after)
            tops, low = [None] * size, None
            for q in range(vecs):
                value = state_b[t, q] * scale[t]
                for i in down:
                    value = value + adds[i]
                    if score:
                        part = kept[t, at + i, q] * value
                        tops[i] = part if q == 0 else tops[i] + part
                        if i == size - 1:
                            part = kept_low[t, g * blocks + n, q] * value
                            low = part if q == 0 else low + part
                    else:
                        waiting[t, n * size + i, q] = value
                    value = emit[t, at + i, q] * value
                state_b[t, q] = value
            if score:
                put_sums(t, g, n, tops, low)
        return tuple(result)

    def score_waiting(g, n):
        at = g * slots + n * size
        end = n * size + size - 1
        for t in team:
            tops = [total(kept[t, at + i, q] * waiting[t, n * size + i, q] for q in range(vecs)) for i in range(size)]
            put_sums(t, g, n, tops, total(kept_low[t, g * blocks + n, q] * waiting[t, end, q] for q in range(vecs)))

    def out_copy(g, from_g):
        return pltpu.make_async_remote_copy(
            src_ref=dos.at[g], dst_ref=out_recv.at[from_g], send_sem=out_send.at[g],
            recv_sem=out_recv_sem.at[from_g], device_id=(g, h_me), device_id_type=MESH)

    row_at = lax.broadcasted_iota(jnp.int32, (slots, LANE), 0)
    own_lane = (lax.broadcasted_iota(jnp.int32, (slots, LANE), 1) == row_at) & (row_at < local_m)

    def finish(g):
        result = jnp.zeros((SUB, LANE), jnp.float32)
        for t in team:
            def gathered(sums):
                parts = [sums[t, pl.ds(g * slots * SUB + k, slots, stride=SUB), :] for k in range(SUB)]
                return jnp.sum(total(parts), axis=1, keepdims=True)

            value = jnp.broadcast_to(gathered(numer) / gathered(denom), (slots, LANE))
            value = jnp.sum(jnp.where(own_lane, value, 0.0), axis=0, keepdims=True)
            result = jnp.where(sub_at == g_me * each + t, jnp.broadcast_to(value, (SUB, LANE)), result)
        dos[g] = result
        pl.when(g != g_me)(lambda: out_copy(g, g_me).start())

    @pl.when(active)
    def _():
        for load in loads[3:]:
            load.wait()
        scale_a = arrange(0, state_a)
        scale_b = arrange(1, state_b)
        table[2 * each, end_row:end_row + SUB, :] = jnp.zeros((SUB, LANE), jnp.float32)

        def first_pass(g, scale):
            read_meta(g)
            expand(g)
            for n in range(blocks):
                prepare(g, n)
                scale = step_a(g, n, scale)
            return scale

        scale_a = lax.fori_loop(0, far, first_pass, scale_a)
        read_meta(far)
        expand(far)
        ready = set()
        for n in range(blocks):
            for k in (n, blocks - 1 - n):
                if k not in ready:
                    ready.add(k)
                    prepare(far, k)
            scale_a = step_a(far, n, scale_a)
            scale_b = step_b(far, blocks - 1 - n, scale_b, False)
        for n in range(blocks):
            score_waiting(far, n)

        def second_pass(k, scale):
            g = far - 1 - k
            finish(g + 1)
            for n in reversed(range(blocks)):
                scale = step_b(g, n, scale, True)
            return scale

        lax.fori_loop(0, far, second_pass, scale_b)
        finish(0)
        out_recv[g_me] = dos[g_me]

    each_send(lambda copy: copy.wait_send())
    for g in range(teams):
        pl.when(g != g_me)(lambda: out_copy(g_me, g).wait_recv())
    result = out_recv[0]
    for g in range(1, teams):
        result = jnp.where(sub_at // each == g, out_recv[g], result)
    out[...] = result[0:targets, 0:local_m]

    @pl.when(active)
    def _():
        each_group(lambda g: pl.when(g != g_me)(lambda: out_copy(g, g_me).wait_send()))


def solution(mesh):
    groups, haps = mesh.shape["grp"], mesh.shape["hap"]

    def local(alleles, observed, map_steps, start_weights, end_weights):
        local_m, local_w = alleles.shape
        targets, total_haps = start_weights.shape
        words = local_w * haps
        bits_word = total_haps // words
        reps = LANE * SUB // words
        vecs = bits_word // reps
        pack = LANE // local_w
        slots = pack * -(-local_m // pack)
        size = block_size(local_m)
        blocks = groups * (local_m // size)
        each = targets_each(targets, groups * slots * total_haps * 4)
        teams = targets // each
        assert targets < SUB and teams <= groups and slots % SUB == 0
        dims = (groups, haps, local_m, targets, words, bits_word)
        f32, i32 = jnp.float32, jnp.int32
        dma = pltpu.SemaphoreType.DMA
        tile = (SUB, LANE)
        out = pl.pallas_call(
            functools.partial(kernel, dims),
            out_shape=pltpu.VMEM((targets, local_m), f32),
            in_specs=[pl.BlockSpec(memory_space=pltpu.HBM)] * 5,
            out_specs=pl.BlockSpec(memory_space=pltpu.VMEM),
            scratch_shapes=[
                pltpu.VMEM((local_m, local_w), i32),
                pltpu.VMEM((targets, local_m), i32),
                pltpu.SMEM((local_m,), i32),
                pltpu.VMEM((slots + SUB, LANE), i32),
                pltpu.VMEM(tile, i32),
                pltpu.VMEM(tile, i32),
                pltpu.VMEM((groups, haps * SUB, LANE), i32),
                pltpu.VMEM((groups, *tile), i32),
                pltpu.VMEM((groups * slots, *tile), i32),
                pltpu.VMEM((2 * each + 1, groups * slots + SUB, LANE), f32),
                pltpu.VMEM((2, targets, total_haps), f32),
                pltpu.VMEM((vecs * SUB * targets, LANE), f32),
                pltpu.VMEM((each, vecs, *tile), f32),
                pltpu.VMEM((each, vecs, *tile), f32),
                pltpu.VMEM((each, groups * slots, vecs, *tile), f32),
                pltpu.VMEM((each, blocks, size * (size + 1) // 2, *tile), f32),
                pltpu.VMEM((each, groups * slots, vecs, *tile), f32),
                pltpu.VMEM((each, blocks, vecs, *tile), f32),
                pltpu.VMEM((each, local_m, vecs, *tile), f32),
                pltpu.VMEM((each, groups * slots * SUB, LANE), f32),
                pltpu.VMEM((each, groups * slots * SUB, LANE), f32),
                pltpu.VMEM((groups, *tile), f32),
                pltpu.VMEM((teams, *tile), f32),
                dma((5,)), dma((teams, haps)), dma((groups, haps)), dma((teams,)), dma((groups,)),
                dma((groups,)), dma((teams,)),
            ],
            compiler_params=pltpu.CompilerParams(
                collective_id=0, has_side_effects=True, vmem_limit_bytes=60 * 1024 * 1024),
        )(alleles, observed.T, map_steps, start_weights, end_weights)
        return out.T

    in_specs = (P("grp", "hap"), P("grp", "hap"), P("grp"), P("hap", None), P("hap", None))
    return jax.shard_map(local, mesh=mesh, in_specs=in_specs, out_specs=P("grp", "hap"), check_vma=False)
```

```python
import functools
import jax
import jax.numpy as jnp
from jax import lax
from jax.experimental import pallas as pl
from jax.experimental.pallas import tpu as pltpu
from jax.sharding import PartitionSpec as P

error_rate = 0.01
map_unit = 100000.0
SUB, LANE = 8, 128
MESH = pl.DeviceIdType.MESH


def total(parts):
    parts = list(parts)
    while len(parts) > 1:
        parts = [a + b for a, b in zip(parts[::2], parts[1::2])] + parts[len(parts) // 2 * 2:]
    return parts[0]


def block_size(local_m):
    return next(n for n in (5, 4, 3, 2, 1) if local_m % n == 0)


def targets_each(targets, state_bytes):
    return 2 if targets % 2 == 0 and 4 * state_bytes <= 40 * 1024 * 1024 else 1


def kernel(dims, alleles, observed, steps, starts, ends, out,
           own_alleles, own_observed, own_steps, tmp, block, meta, recv, metas, bits, table, weights, staged,
           state_a, state_b, emit, runs, kept, kept_low, waiting, numer, denom, dos, out_recv,
           load_sem, send_sem, recv_sem, meta_send, meta_recv, out_send, out_recv_sem):
    groups, haps, local_m, targets, words, bits_word = dims
    total_haps = words * bits_word
    local_w = words // haps
    span = words // SUB
    reps = LANE // span
    vecs = bits_word // reps
    pack = LANE // local_w
    rows = -(-local_m // pack)
    slots = pack * rows
    share = haps // SUB
    size = block_size(local_m)
    blocks = local_m // size
    end_row = groups * slots
    each = targets_each(targets, groups * slots * total_haps * 4)
    teams = targets // each
    far = groups - 1
    g_me, h_me = lax.axis_index("grp"), lax.axis_index("hap")
    active = g_me < teams

    sources = [
        (alleles, own_alleles), (observed, own_observed), (steps, own_steps), (starts, weights.at[0]), (ends, weights.at[1])]
    loads = [pltpu.make_async_copy(source, target, load_sem.at[n]) for n, (source, target) in enumerate(sources)]
    for load in loads[:3]:
        load.start()

    def each_hap(act, first=0):
        if haps <= 8:
            for d in range(first, haps):
                act(lax.rem(h_me + d, haps))
        else:
            pl.loop(first, haps)(lambda d: act(lax.rem(h_me + d, haps)))

    def each_group(act):
        if groups <= 4:
            for g in reversed(range(groups)):
                act(g)
        else:
            pl.loop(0, groups)(lambda k: act(far - k))

    def not_me(g, h, act):
        pl.when((g != g_me) | (h != h_me))(act)

    barrier = pltpu.get_barrier_semaphore()

    def greet(g, h):
        pl.semaphore_signal(barrier, inc=1, device_id=(g, h), device_id_type=MESH)

    @pl.when(active)
    def _():
        each_group(lambda g: each_hap(lambda h: not_me(g, h, lambda: greet(g, h))))
        for load in loads[3:]:
            load.start()

    lane = lax.broadcasted_iota(jnp.int32, (SUB, LANE), 1)
    sub_at = lax.broadcasted_iota(jnp.int32, (SUB, LANE), 0)
    tmp[...] = jnp.zeros_like(tmp)
    for load in loads[:3]:
        load.wait()
    tmp[0:local_m, 0:local_w] = own_alleles[...]
    dense = tmp[0:SUB, :]
    for p in range(1, pack):
        dense = jnp.where(lane // local_w == p, pltpu.roll(tmp[p * rows:p * rows + SUB, :], p * local_w, 1), dense)
    block[...] = dense
    recv[g_me, pl.ds(pl.multiple_of(h_me * SUB, SUB), SUB), :] = dense
    tmp[0:targets, 0:local_m] = own_observed[...]
    columns = tmp[0:SUB, :]
    for i in range(local_m):
        columns = jnp.where((sub_at == targets) & (lane == i), own_steps[i], columns)
    meta[...] = columns
    metas[g_me] = columns

    def block_copy(g, h, from_g, from_h):
        return pltpu.make_async_remote_copy(
            src_ref=block, dst_ref=recv.at[from_g, pl.ds(pl.multiple_of(from_h * SUB, SUB), SUB), :],
            send_sem=send_sem.at[g, h], recv_sem=recv_sem.at[from_g, from_h],
            device_id=(g, h), device_id_type=MESH)

    def meta_copy(g, from_g):
        return pltpu.make_async_remote_copy(
            src_ref=meta, dst_ref=metas.at[from_g], send_sem=meta_send.at[g], recv_sem=meta_recv.at[from_g],
            device_id=(g, h_me), device_id_type=MESH)

    def each_send(act):
        for g in range(teams):
            pl.when(g != g_me)(lambda: act(meta_copy(g, g_me)))
            each_hap(lambda h: not_me(g, h, lambda: act(block_copy(g, h, g_me, h_me))))

    pl.semaphore_wait(barrier, teams * haps - jnp.where(active, 1, 0))
    each_send(lambda copy: copy.start())

    def add_up(value):
        for shift in (4, 2, 1):
            value = value + pltpu.roll(value, shift, 0)
        return jnp.broadcast_to(jnp.sum(value, axis=1, keepdims=True), (SUB, LANE))

    def arrange(which, state):
        for r in range(vecs):
            for s in range(SUB):
                at = s * vecs + r
                staged[at * targets:(at + 1) * targets, :] = weights[which, :, at * LANE:(at + 1) * LANE]
        first = g_me * each
        sums = [None] * each
        for q in range(vecs):
            spot = bits_word * (lane % span) + reps * q + lane // span
            chosen, within = spot // LANE, spot % LANE
            value = [jnp.zeros((SUB, LANE), jnp.float32)] * each
            for r in range(vecs):
                here = chosen == r
                for t in range(each):
                    source = staged[pl.ds(r * targets + first + t, SUB, stride=vecs * targets), :]
                    moved = jnp.take_along_axis(source, within, axis=1, mode="promise_in_bounds")
                    value[t] = jnp.where(here, moved, value[t])
            for t in range(each):
                state[t, q] = value[t]
                sums[t] = value[t] if q == 0 else sums[t] + value[t]
        return tuple(1.0 / add_up(sums[t]) for t in range(each))

    def read_meta(g):
        pl.when(g != g_me)(lambda: meta_copy(g_me, g).wait_recv())
        same = lax.broadcasted_iota(jnp.int32, (slots, LANE), 0) == lax.broadcasted_iota(jnp.int32, (slots, LANE), 1)

        def turned(at):
            values = jnp.broadcast_to(metas[g, pl.ds(at, 1), :].astype(jnp.float32), (slots, LANE))
            summed = jnp.sum(jnp.where(same, values, 0.0), axis=1, keepdims=True)
            return jnp.broadcast_to(summed, (slots, LANE))

        at = pl.ds(pl.multiple_of(g * slots, SUB), slots)
        for t in range(each):
            seen = turned(g_me * each + t)
            table[2 * t, at, :] = jnp.where(seen == 2.0, 1.0, jnp.where(seen == 1.0, 1.0 - error_rate, error_rate))
            table[2 * t + 1, at, :] = jnp.where(seen == 2.0, 1.0, jnp.where(seen == 0.0, 1.0 - error_rate, error_rate))
        rate = 1.0 - jnp.exp(-turned(targets) / map_unit)
        table[2 * each, at, :] = (rate / total_haps) / (1.0 - rate)

    def expand(g):
        each_hap(lambda h: not_me(g, h, lambda: block_copy(g_me, h_me, g, h).wait_recv()))
        for r in range(rows):
            parts = [recv[g, pl.ds(j * SUB + r, SUB, stride=SUB * share), :] for j in range(share)]
            for p in range(pack):
                n = p * rows + r
                if n >= local_m:
                    continue
                value = jnp.zeros((SUB, LANE), jnp.int32)
                for e in range(reps):
                    for j in range(share):
                        begin = e * span + j * local_w
                        shift = (begin - p * local_w) % LANE
                        piece = parts[j] if shift == 0 else pltpu.roll(parts[j], shift, 1)
                        piece = piece if e == 0 else jnp.right_shift(piece, e)
                        value = jnp.where((lane >= begin) & (lane < begin + local_w), piece, value)
                bits[g * slots + n] = value

    def row(kind, slot):
        return jnp.broadcast_to(table[kind, pl.ds(slot, 1), :], (SUB, LANE))

    def masked(words_in, q):
        return jnp.bitwise_and(words_in, 1 << (reps * q)) != 0

    pairs = [(j, i) for j in range(size) for i in range(j, size)]
    team = range(each)

    def prepare(g, n):
        at = g * slots + n * size
        words_in = [bits[at + i] for i in range(size)]
        for t in team:
            tops = [(row(2 * t, at + i), row(2 * t + 1, at + i)) for i in range(size)]
            for q in range(vecs):
                for i in range(size):
                    emit[t, at + i, q] = jnp.where(masked(words_in[i], q), *tops[i])

    inner = min(size, 4)
    used = sum(1 << (reps * q) for q in range(vecs))

    def count_patterns(g):
        counts = [jnp.zeros((SUB, LANE), jnp.float32)] * (1 << (size - inner))
        for n in range(blocks):
            sets = [jnp.full((SUB, LANE), used, jnp.int32)]
            for i in range(size):
                word = bits[g * slots + n * size + i]
                other = jnp.bitwise_not(word)
                sets = [jnp.bitwise_and(x, other) for x in sets] + [jnp.bitwise_and(x, word) for x in sets]
            sets += [jnp.zeros((SUB, LANE), jnp.int32)] * (LANE // SUB - len(sets))
            held = jnp.concatenate([lax.population_count(x).astype(jnp.float32) for x in sets], axis=0)
            found = lax.dot_general(
                jnp.ones((SUB, LANE), jnp.bfloat16), held.astype(jnp.bfloat16), (((1,), (1,)), ((), ())),
                preferred_element_type=jnp.float32)
            counts = [jnp.where(sub_at == n, found[:, k * LANE:(k + 1) * LANE], c) for k, c in enumerate(counts)]
        return counts

    def make_spans(g):
        counts = count_patterns(g)
        pattern = lane // SUB
        for t in team:
            def rows_of(kind, i):
                return table[kind, pl.ds(g * slots + i, SUB, stride=size), :]

            e = [
                jnp.where(jnp.bitwise_and(jnp.right_shift(pattern, i), 1) != 0, rows_of(2 * t, i), rows_of(2 * t + 1, i))
                for i in range(inner)
            ]
            whole = total(counts)
            if size > inner:
                last = counts[0] * rows_of(2 * t + 1, inner) + counts[1] * rows_of(2 * t, inner)
            for j in range(size):
                run = None
                for i in range(j, size):
                    if i < inner:
                        run = e[i] if run is None else run * e[i]
                        value = whole * run
                    else:
                        value = last if run is None else last * run
                    summed = jnp.broadcast_to(jnp.sum(value, axis=1, keepdims=True), (SUB, LANE))
                    runs[t, g, pairs.index((j, i))] = summed

    def ahead(t, state, g, n, order):
        at = g * slots + n * size
        sums = [None] * size
        for q in range(vecs):
            value = state[t, q]
            for i in order:
                value = value * emit[t, at + i, q]
                sums[i] = value if q == 0 else sums[i] + value
        return [add_up(value) for value in sums]

    def solve(t, sums, scale, g, n, order, after):
        at = g * slots + n * size
        span_of = {
            pair: jnp.broadcast_to(runs[t, g, k, pl.ds(n, 1), :], (SUB, LANE)) for k, pair in enumerate(pairs)}
        adds = {}
        last = None
        for i in order:
            slot = at + i
            if after:
                slot = slot + 1
                if i == size - 1:
                    ahead = jnp.where(g + 1 < groups, (g + 1) * slots, end_row)
                    slot = jnp.where(n * size + size == local_m, ahead, slot)
            adds[i] = row(2 * each, slot) if last is None else row(2 * each, slot) * last
            last = sums[i] * scale
            for j in adds:
                last = last + adds[j] * span_of[min(i, j), max(i, j)]
        return adds, 1.0 / last

    up, down = list(range(size)), list(range(size))[::-1]

    def step_a(g, n, scale):
        at = g * slots + n * size
        sums = [ahead(t, state_a, g, n, up) for t in team]
        solved = [solve(t, sums[t], scale[t], g, n, up, False) for t in team]
        words_in = [bits[at + i] for i in range(size)]
        for q in range(vecs):
            masks = [masked(words_in[i], q) for i in range(size)]
            for t in team:
                value = state_a[t, q] * scale[t]
                for i in up:
                    value = emit[t, at + i, q] * (value + solved[t][0][i])
                    kept[t, at + i, q] = jnp.where(masks[i], value, 0.0)
                kept_low[t, g * blocks + n, q] = value
                state_a[t, q] = value
        return tuple(solved[t][1] for t in team)

    def put_sums(t, g, n, tops, low):
        for i in range(size):
            at = pl.ds(pl.multiple_of((g * slots + n * size + i) * SUB, SUB), SUB)
            numer[t, at, :] = tops[i]
            denom[t, at, :] = low

    def step_b(g, n, scale, earlier):
        at = g * slots + n * size
        sums = [ahead(t, state_b, g, n, down) for t in team]
        if earlier is not None:
            score_waiting(*earlier)
        solved = [solve(t, sums[t], scale[t], g, n, down, True) for t in team]
        for t in team:
            for q in range(vecs):
                value = state_b[t, q] * scale[t]
                for i in down:
                    value = value + solved[t][0][i]
                    waiting[t, n * size + i, q] = value
                    value = emit[t, at + i, q] * value
                state_b[t, q] = value
        return tuple(solved[t][1] for t in team)

    def score_waiting(g, n):
        at = g * slots + n * size
        end = n * size + size - 1
        for t in team:
            tops, low = [None] * size, None
            for q in range(vecs):
                for i in range(size):
                    part = kept[t, at + i, q] * waiting[t, n * size + i, q]
                    tops[i] = part if q == 0 else tops[i] + part
                part = kept_low[t, g * blocks + n, q] * waiting[t, end, q]
                low = part if q == 0 else low + part
            put_sums(t, g, n, tops, low)

    def out_copy(g, from_g):
        return pltpu.make_async_remote_copy(
            src_ref=dos.at[g], dst_ref=out_recv.at[from_g], send_sem=out_send.at[g],
            recv_sem=out_recv_sem.at[from_g], device_id=(g, h_me), device_id_type=MESH)

    row_at = lax.broadcasted_iota(jnp.int32, (slots, LANE), 0)
    own_lane = (lax.broadcasted_iota(jnp.int32, (slots, LANE), 1) == row_at) & (row_at < local_m)

    def finish(g):
        result = jnp.zeros((SUB, LANE), jnp.float32)
        for t in team:
            def gathered(sums):
                parts = [sums[t, pl.ds(g * slots * SUB + k, slots, stride=SUB), :] for k in range(SUB)]
                return jnp.sum(total(parts), axis=1, keepdims=True)

            value = jnp.broadcast_to(gathered(numer) / gathered(denom), (slots, LANE))
            value = jnp.sum(jnp.where(own_lane, value, 0.0), axis=0, keepdims=True)
            result = jnp.where(sub_at == g_me * each + t, jnp.broadcast_to(value, (SUB, LANE)), result)
        dos[g] = result
        pl.when(g != g_me)(lambda: out_copy(g, g_me).start())

    @pl.when(active)
    def _():
        for load in loads[3:]:
            load.wait()
        scale_a = arrange(0, state_a)
        scale_b = arrange(1, state_b)
        table[2 * each, end_row:end_row + SUB, :] = jnp.zeros((SUB, LANE), jnp.float32)

        def first_pass(g, scale):
            read_meta(g)
            expand(g)
            make_spans(g)
            for n in range(blocks):
                prepare(g, n)
                scale = step_a(g, n, scale)
            return scale

        scale_a = lax.fori_loop(0, far, first_pass, scale_a)
        read_meta(far)
        expand(far)
        make_spans(far)
        ready = set()
        for n in range(blocks):
            for k in (n, blocks - 1 - n):
                if k not in ready:
                    ready.add(k)
                    prepare(far, k)
            scale_a = step_a(far, n, scale_a)
            scale_b = step_b(far, blocks - 1 - n, scale_b, None)
        for n in range(1, blocks):
            score_waiting(far, n)

        def second_pass(k, scale):
            g = far - 1 - k
            for n in reversed(range(blocks)):
                scale = step_b(g, n, scale, (g, n + 1) if n + 1 < blocks else (g + 1, 0))
                if n + 1 == blocks:
                    finish(g + 1)
            return scale

        lax.fori_loop(0, far, second_pass, scale_b)
        score_waiting(0, 0)
        finish(0)
        out_recv[g_me] = dos[g_me]

    each_send(lambda copy: copy.wait_send())
    for g in range(teams):
        pl.when(g != g_me)(lambda: out_copy(g_me, g).wait_recv())
    result = out_recv[0]
    for g in range(1, teams):
        result = jnp.where(sub_at // each == g, out_recv[g], result)
    out[...] = result[0:targets, 0:local_m]

    @pl.when(active)
    def _():
        each_group(lambda g: pl.when(g != g_me)(lambda: out_copy(g, g_me).wait_send()))


def solution(mesh):
    groups, haps = mesh.shape["grp"], mesh.shape["hap"]

    def local(alleles, observed, map_steps, start_weights, end_weights):
        local_m, local_w = alleles.shape
        targets, total_haps = start_weights.shape
        words = local_w * haps
        bits_word = total_haps // words
        reps = LANE * SUB // words
        vecs = bits_word // reps
        pack = LANE // local_w
        slots = pack * -(-local_m // pack)
        size = block_size(local_m)
        blocks = groups * (local_m // size)
        each = targets_each(targets, groups * slots * total_haps * 4)
        teams = targets // each
        assert targets < SUB and teams <= groups and slots % SUB == 0
        dims = (groups, haps, local_m, targets, words, bits_word)
        f32, i32 = jnp.float32, jnp.int32
        dma = pltpu.SemaphoreType.DMA
        tile = (SUB, LANE)
        out = pl.pallas_call(
            functools.partial(kernel, dims),
            out_shape=pltpu.VMEM((targets, local_m), f32),
            in_specs=[pl.BlockSpec(memory_space=pltpu.HBM)] * 5,
            out_specs=pl.BlockSpec(memory_space=pltpu.VMEM),
            scratch_shapes=[
                pltpu.VMEM((local_m, local_w), i32),
                pltpu.VMEM((targets, local_m), i32),
                pltpu.SMEM((local_m,), i32),
                pltpu.VMEM((slots + SUB, LANE), i32),
                pltpu.VMEM(tile, i32),
                pltpu.VMEM(tile, i32),
                pltpu.VMEM((groups, haps * SUB, LANE), i32),
                pltpu.VMEM((groups, *tile), i32),
                pltpu.VMEM((groups * slots, *tile), i32),
                pltpu.VMEM((2 * each + 1, groups * slots + (size + 1) * SUB, LANE), f32),
                pltpu.VMEM((2, targets, total_haps), f32),
                pltpu.VMEM((vecs * SUB * targets, LANE), f32),
                pltpu.VMEM((each, vecs, *tile), f32),
                pltpu.VMEM((each, vecs, *tile), f32),
                pltpu.VMEM((each, groups * slots, vecs, *tile), f32),
                pltpu.VMEM((each, groups, size * (size + 1) // 2, *tile), f32),
                pltpu.VMEM((each, groups * slots, vecs, *tile), f32),
                pltpu.VMEM((each, blocks, vecs, *tile), f32),
                pltpu.VMEM((each, local_m, vecs, *tile), f32),
                pltpu.VMEM((each, groups * slots * SUB, LANE), f32),
                pltpu.VMEM((each, groups * slots * SUB, LANE), f32),
                pltpu.VMEM((groups, *tile), f32),
                pltpu.VMEM((teams, *tile), f32),
                dma((5,)), dma((teams, haps)), dma((groups, haps)), dma((teams,)), dma((groups,)),
                dma((groups,)), dma((teams,)),
            ],
            compiler_params=pltpu.CompilerParams(
                collective_id=0, has_side_effects=True, vmem_limit_bytes=60 * 1024 * 1024),
        )(alleles, observed.T, map_steps, start_weights, end_weights)
        return out.T

    in_specs = (P("grp", "hap"), P("grp", "hap"), P("grp"), P("hap", None), P("hap", None))
    return jax.shard_map(local, mesh=mesh, in_specs=in_specs, out_specs=P("grp", "hap"), check_vma=False)
```

```python
import functools
import jax
import jax.numpy as jnp
from jax import lax
from jax.experimental import pallas as pl
from jax.experimental.pallas import tpu as pltpu
from jax.sharding import PartitionSpec as P

error_rate = 0.01
map_unit = 100000.0
SUB, LANE = 8, 128
MESH = pl.DeviceIdType.MESH


def total(parts):
    parts = list(parts)
    while len(parts) > 1:
        parts = [a + b for a, b in zip(parts[::2], parts[1::2])] + parts[len(parts) // 2 * 2:]
    return parts[0]


def block_size(local_m):
    return next(n for n in (5, 4, 3, 2, 1) if local_m % n == 0)


def split_targets(targets, state_bytes):
    if targets > 1 and 2 * (targets - 1) * state_bytes <= 40 * 1024 * 1024:
        return targets // 2, targets - targets // 2
    return (1,) * targets


def kernel(dims, alleles, observed, steps, starts, ends, out,
           own_alleles, own_observed, own_steps, tmp, block, meta, recv, metas, bits, table, weights, staged,
           state_a, state_b, emit, runs, kept, kept_low, waiting, numer, denom, dos, out_recv,
           load_sem, send_sem, recv_sem, meta_send, meta_recv, out_send, out_recv_sem):
    groups, haps, local_m, targets, words, bits_word = dims
    total_haps = words * bits_word
    local_w = words // haps
    span = words // SUB
    reps = LANE // span
    vecs = bits_word // reps
    pack = LANE // local_w
    rows = -(-local_m // pack)
    slots = pack * rows
    share = haps // SUB
    size = block_size(local_m)
    blocks = local_m // size
    end_row = groups * slots
    split = split_targets(targets, groups * slots * total_haps * 4)
    teams = len(split)
    far = groups - 1
    g_me, h_me = lax.axis_index("grp"), lax.axis_index("hap")
    active = g_me < teams

    sources = [
        (alleles, own_alleles), (observed, own_observed), (steps, own_steps), (starts, weights.at[0]), (ends, weights.at[1])]
    loads = [pltpu.make_async_copy(source, target, load_sem.at[n]) for n, (source, target) in enumerate(sources)]
    for load in loads[:3]:
        load.start()

    def each_hap(act, first=0):
        if haps <= 8:
            for d in range(first, haps):
                act(lax.rem(h_me + d, haps))
        else:
            pl.loop(first, haps)(lambda d: act(lax.rem(h_me + d, haps)))

    def each_group(act):
        if groups <= 4:
            for g in reversed(range(groups)):
                act(g)
        else:
            pl.loop(0, groups)(lambda k: act(far - k))

    def not_me(g, h, act):
        pl.when((g != g_me) | (h != h_me))(act)

    barrier = pltpu.get_barrier_semaphore()

    def greet(g, h):
        pl.semaphore_signal(barrier, inc=1, device_id=(g, h), device_id_type=MESH)

    @pl.when(active)
    def _():
        each_group(lambda g: each_hap(lambda h: not_me(g, h, lambda: greet(g, h))))
        for load in loads[3:]:
            load.start()

    lane = lax.broadcasted_iota(jnp.int32, (SUB, LANE), 1)
    sub_at = lax.broadcasted_iota(jnp.int32, (SUB, LANE), 0)
    tmp[...] = jnp.zeros_like(tmp)
    for load in loads[:3]:
        load.wait()
    tmp[0:local_m, 0:local_w] = own_alleles[...]
    dense = tmp[0:SUB, :]
    for p in range(1, pack):
        dense = jnp.where(lane // local_w == p, pltpu.roll(tmp[p * rows:p * rows + SUB, :], p * local_w, 1), dense)
    block[...] = dense
    recv[g_me, pl.ds(pl.multiple_of(h_me * SUB, SUB), SUB), :] = dense
    tmp[0:targets, 0:local_m] = own_observed[...]
    columns = tmp[0:SUB, :]
    for i in range(local_m):
        columns = jnp.where((sub_at == targets) & (lane == i), own_steps[i], columns)
    meta[...] = columns
    metas[g_me] = columns

    def block_copy(g, h, from_g, from_h):
        return pltpu.make_async_remote_copy(
            src_ref=block, dst_ref=recv.at[from_g, pl.ds(pl.multiple_of(from_h * SUB, SUB), SUB), :],
            send_sem=send_sem.at[g, h], recv_sem=recv_sem.at[from_g, from_h],
            device_id=(g, h), device_id_type=MESH)

    def meta_copy(g, from_g):
        return pltpu.make_async_remote_copy(
            src_ref=meta, dst_ref=metas.at[from_g], send_sem=meta_send.at[g], recv_sem=meta_recv.at[from_g],
            device_id=(g, h_me), device_id_type=MESH)

    def each_send(act):
        for g in reversed(range(teams)):
            pl.when(g != g_me)(lambda: act(meta_copy(g, g_me)))
            each_hap(lambda h: not_me(g, h, lambda: act(block_copy(g, h, g_me, h_me))))

    pl.semaphore_wait(barrier, teams * haps - jnp.where(active, 1, 0))
    each_send(lambda copy: copy.start())

    def out_copy(g, from_g):
        return pltpu.make_async_remote_copy(
            src_ref=dos.at[g], dst_ref=out_recv.at[from_g], send_sem=out_send.at[g],
            recv_sem=out_recv_sem.at[from_g], device_id=(g, h_me), device_id_type=MESH)

    def run(first, each):
        def add_up(value):
            for shift in (4, 2, 1):
                value = value + pltpu.roll(value, shift, 0)
            return jnp.broadcast_to(jnp.sum(value, axis=1, keepdims=True), (SUB, LANE))

        def arrange(which, state):
            for r in range(vecs):
                for s in range(SUB):
                    at = s * vecs + r
                    staged[at * targets:(at + 1) * targets, :] = weights[which, :, at * LANE:(at + 1) * LANE]
            sums = [None] * each
            for q in range(vecs):
                spot = bits_word * (lane % span) + reps * q + lane // span
                chosen, within = spot // LANE, spot % LANE
                value = [jnp.zeros((SUB, LANE), jnp.float32)] * each
                for r in range(vecs):
                    here = chosen == r
                    for t in range(each):
                        source = staged[pl.ds(r * targets + first + t, SUB, stride=vecs * targets), :]
                        moved = jnp.take_along_axis(source, within, axis=1, mode="promise_in_bounds")
                        value[t] = jnp.where(here, moved, value[t])
                for t in range(each):
                    state[t, q] = value[t]
                    sums[t] = value[t] if q == 0 else sums[t] + value[t]
            return tuple(1.0 / add_up(sums[t]) for t in range(each))

        def arrived(g):
            pl.when(g != g_me)(lambda: meta_copy(g_me, g).wait_recv())
            each_hap(lambda h: not_me(g, h, lambda: block_copy(g_me, h_me, g, h).wait_recv()))

        def read_meta(g):
            same = lax.broadcasted_iota(jnp.int32, (slots, LANE), 0) == lax.broadcasted_iota(jnp.int32, (slots, LANE), 1)

            def turned(at):
                values = jnp.broadcast_to(metas[g, pl.ds(at, 1), :].astype(jnp.float32), (slots, LANE))
                summed = jnp.sum(jnp.where(same, values, 0.0), axis=1, keepdims=True)
                return jnp.broadcast_to(summed, (slots, LANE))

            at = pl.ds(pl.multiple_of(g * slots, SUB), slots)
            for t in range(each):
                seen = turned(first + t)
                table[2 * t, at, :] = jnp.where(seen == 2.0, 1.0, jnp.where(seen == 1.0, 1.0 - error_rate, error_rate))
                table[2 * t + 1, at, :] = jnp.where(seen == 2.0, 1.0, jnp.where(seen == 0.0, 1.0 - error_rate, error_rate))
            rate = 1.0 - jnp.exp(-turned(targets) / map_unit)
            table[2 * each, at, :] = (rate / total_haps) / (1.0 - rate)

        def expand(g):
            for r in range(rows):
                parts = [recv[g, pl.ds(j * SUB + r, SUB, stride=SUB * share), :] for j in range(share)]
                for p in range(pack):
                    n = p * rows + r
                    if n >= local_m:
                        continue
                    value = jnp.zeros((SUB, LANE), jnp.int32)
                    for e in range(reps):
                        for j in range(share):
                            begin = e * span + j * local_w
                            shift = (begin - p * local_w) % LANE
                            piece = parts[j] if shift == 0 else pltpu.roll(parts[j], shift, 1)
                            piece = piece if e == 0 else jnp.right_shift(piece, e)
                            value = jnp.where((lane >= begin) & (lane < begin + local_w), piece, value)
                    bits[g * slots + n] = value

        def row(kind, slot):
            return jnp.broadcast_to(table[kind, pl.ds(slot, 1), :], (SUB, LANE))

        def masked(words_in, q):
            return jnp.bitwise_and(words_in, 1 << (reps * q)) != 0

        pairs = [(j, i) for j in range(size) for i in range(j, size)]
        team = range(each)

        def prepare(g, n):
            at = g * slots + n * size
            words_in = [bits[at + i] for i in range(size)]
            for t in team:
                tops = [(row(2 * t, at + i), row(2 * t + 1, at + i)) for i in range(size)]
                for q in range(vecs):
                    for i in range(size):
                        mask = masked(words_in[i], q)
                        emit[t, at + i, q] = jnp.where(mask, *tops[i])
                        kept[t, at + i, q] = jnp.where(mask, tops[i][0], 0.0)

        inner = min(size, 4)
        used = sum(1 << (reps * q) for q in range(vecs))

        def count_patterns(g):
            counts = [jnp.zeros((SUB, LANE), jnp.float32)] * (1 << (size - inner))
            for n in range(blocks):
                sets = [jnp.full((SUB, LANE), used, jnp.int32)]
                for i in range(size):
                    word = bits[g * slots + n * size + i]
                    other = jnp.bitwise_not(word)
                    sets = [jnp.bitwise_and(x, other) for x in sets] + [jnp.bitwise_and(x, word) for x in sets]
                sets += [jnp.zeros((SUB, LANE), jnp.int32)] * (LANE // SUB - len(sets))
                held = jnp.concatenate([lax.population_count(x).astype(jnp.float32) for x in sets], axis=0)
                found = lax.dot_general(
                    jnp.ones((SUB, LANE), jnp.bfloat16), held.astype(jnp.bfloat16), (((1,), (1,)), ((), ())),
                    preferred_element_type=jnp.float32)
                counts = [jnp.where(sub_at == n, found[:, k * LANE:(k + 1) * LANE], c) for k, c in enumerate(counts)]
            return counts

        def make_spans(g):
            counts = count_patterns(g)
            pattern = lane // SUB
            for t in team:
                def rows_of(kind, i):
                    return table[kind, pl.ds(g * slots + i, SUB, stride=size), :]

                e = [
                    jnp.where(jnp.bitwise_and(jnp.right_shift(pattern, i), 1) != 0, rows_of(2 * t, i), rows_of(2 * t + 1, i))
                    for i in range(inner)
                ]
                whole = total(counts)
                if size > inner:
                    last = counts[0] * rows_of(2 * t + 1, inner) + counts[1] * rows_of(2 * t, inner)
                for j in range(size):
                    run = None
                    for i in range(j, size):
                        if i < inner:
                            run = e[i] if run is None else run * e[i]
                            value = whole * run
                        else:
                            value = last if run is None else last * run
                        summed = jnp.broadcast_to(jnp.sum(value, axis=1, keepdims=True), (SUB, LANE))
                        runs[t, g, pairs.index((j, i))] = summed

        def ahead(t, state, g, n, order):
            at = g * slots + n * size
            sums = [None] * size
            for q in range(vecs):
                value = state[t, q]
                for i in order:
                    value = value * emit[t, at + i, q]
                    sums[i] = value if q == 0 else sums[i] + value
            return [add_up(value) for value in sums]

        def solve(t, sums, scale, g, n, order, after):
            at = g * slots + n * size
            span_of = {
                pair: jnp.broadcast_to(runs[t, g, k, pl.ds(n, 1), :], (SUB, LANE)) for k, pair in enumerate(pairs)}
            adds = {}
            last = None
            for i in order:
                slot = at + i
                if after:
                    slot = slot + 1
                    if i == size - 1:
                        ahead = jnp.where(g + 1 < groups, (g + 1) * slots, end_row)
                        slot = jnp.where(n * size + size == local_m, ahead, slot)
                adds[i] = row(2 * each, slot) if last is None else row(2 * each, slot) * last
                last = sums[i] * scale
                for j in adds:
                    last = last + adds[j] * span_of[min(i, j), max(i, j)]
            return adds, 1.0 / last

        up, down = list(range(size)), list(range(size))[::-1]

        def prepare_ahead(g, n):
            at = g * slots + n * size
            words_in = [bits[at + i] for i in range(size)]
            sums = [[None] * size for t in team]
            tops = [[(row(2 * t, at + i), row(2 * t + 1, at + i)) for i in range(size)] for t in team]
            for q in range(vecs):
                masks = [masked(words_in[i], q) for i in range(size)]
                for t in team:
                    value = state_a[t, q]
                    for i in up:
                        e = jnp.where(masks[i], *tops[t][i])
                        emit[t, at + i, q] = e
                        kept[t, at + i, q] = jnp.where(masks[i], tops[t][i][0], 0.0)
                        value = value * e
                        sums[t][i] = value if q == 0 else sums[t][i] + value
            return [[add_up(value) for value in sums[t]] for t in team]

        def step_a(g, n, scale, fresh):
            at = g * slots + n * size
            sums = prepare_ahead(g, n) if fresh else [ahead(t, state_a, g, n, up) for t in team]
            solved = [solve(t, sums[t], scale[t], g, n, up, False) for t in team]
            for t in team:
                for q in range(vecs):
                    value = state_a[t, q] * scale[t]
                    for i in up:
                        moved = value + solved[t][0][i]
                        kept[t, at + i, q] = kept[t, at + i, q] * moved
                        value = emit[t, at + i, q] * moved
                    kept_low[t, g * blocks + n, q] = value
                    state_a[t, q] = value
            return tuple(solved[t][1] for t in team)

        def put_sums(t, g, n, tops, low):
            for i in range(size):
                at = pl.ds(pl.multiple_of((g * slots + n * size + i) * SUB, SUB), SUB)
                numer[t, at, :] = tops[i]
                denom[t, at, :] = low

        def step_b(t, g, n, scale, sums, score):
            at = g * slots + n * size
            adds, after = solve(t, sums, scale, g, n, down, True)
            tops, low = [None] * size, None
            for q in range(vecs):
                value = state_b[t, q] * scale
                for i in down:
                    value = value + adds[i]
                    if not score:
                        waiting[t, n * size + i, q] = value
                    else:
                        part = kept[t, at + i, q] * value
                        tops[i] = part if q == 0 else tops[i] + part
                        if i == size - 1:
                            part = kept_low[t, g * blocks + n, q] * value
                            low = part if q == 0 else low + part
                    value = emit[t, at + i, q] * value
                state_b[t, q] = value
            if score:
                put_sums(t, g, n, tops, low)
            return after

        def score_waiting(g, n):
            at = g * slots + n * size
            end = n * size + size - 1
            for t in team:
                tops, low = [None] * size, None
                for q in range(vecs):
                    for i in range(size):
                        part = kept[t, at + i, q] * waiting[t, n * size + i, q]
                        tops[i] = part if q == 0 else tops[i] + part
                    part = kept_low[t, g * blocks + n, q] * waiting[t, end, q]
                    low = part if q == 0 else low + part
                put_sums(t, g, n, tops, low)

        row_at = lax.broadcasted_iota(jnp.int32, (slots, LANE), 0)
        own_lane = (lax.broadcasted_iota(jnp.int32, (slots, LANE), 1) == row_at) & (row_at < local_m)

        def finish(g):
            result = jnp.zeros((SUB, LANE), jnp.float32)
            for t in team:
                def gathered(sums):
                    parts = [sums[t, pl.ds(g * slots * SUB + k, slots, stride=SUB), :] for k in range(SUB)]
                    return jnp.sum(total(parts), axis=1, keepdims=True)

                value = jnp.broadcast_to(gathered(numer) / gathered(denom), (slots, LANE))
                value = jnp.sum(jnp.where(own_lane, value, 0.0), axis=0, keepdims=True)
                result = jnp.where(sub_at == first + t, jnp.broadcast_to(value, (SUB, LANE)), result)
            dos[g] = result
            pl.when(g != g_me)(lambda: out_copy(g, g_me).start())

        for load in loads[3:]:
            load.wait()
        scale_a = arrange(0, state_a)
        scale_b = arrange(1, state_b)
        table[2 * each, end_row:end_row + SUB, :] = jnp.zeros((SUB, LANE), jnp.float32)

        def first_pass(g, scale):
            arrived(g)
            expand(g)
            read_meta(g)
            make_spans(g)
            for n in range(blocks):
                scale = step_a(g, n, scale, True)
            return scale

        scale_a = lax.fori_loop(0, far, first_pass, scale_a)
        arrived(far)
        expand(far)
        read_meta(far)
        make_spans(far)
        ready = set()
        for n in range(blocks):
            m = blocks - 1 - n
            if m != n and m not in ready:
                prepare(far, m)
            scale_a = step_a(far, n, scale_a, n not in ready)
            ready |= {n, m}
            sums = [ahead(t, state_b, far, m, down) for t in team]
            scale_b = tuple(step_b(t, far, m, scale_b[t], sums[t], False) for t in team)

        sums = ahead(0, state_b, far - 1, blocks - 1, down)
        for n in range(blocks):
            score_waiting(far, n)

        def second_pass(k, carry):
            g = far - 1 - k
            scale, sums = list(carry[0]), list(carry[1])
            for n in reversed(range(blocks)):
                scale[0] = step_b(0, g, n, scale[0], sums, True)
                if n:
                    sums = ahead(0, state_b, g, n - 1, down)
                elif groups > 4 or g > 0:
                    sums = ahead(0, state_b, jnp.maximum(g - 1, 0) if groups > 4 else g - 1, blocks - 1, down)
                for t in range(1, each):
                    scale[t] = step_b(t, g, n, scale[t], ahead(t, state_b, g, n, down), True)
                if n + 1 == blocks:
                    finish(g + 1)
            return tuple(scale), tuple(sums)

        carry = scale_b, tuple(sums)
        if groups <= 4:
            for k in range(far):
                carry = second_pass(k, carry)
        else:
            lax.fori_loop(0, far, second_pass, carry)
        finish(0)
        out_recv[g_me] = dos[g_me]

    if len(set(split)) == 1:
        pl.when(active)(lambda: run(g_me * split[0], split[0]))
    else:
        for g in range(teams):
            pl.when(g_me == g)(functools.partial(run, sum(split[:g]), split[g]))

    each_send(lambda copy: copy.wait_send())
    for g in range(teams):
        pl.when(g != g_me)(lambda: out_copy(g_me, g).wait_recv())
    result = out_recv[0]
    for g in range(1, teams):
        result = jnp.where(sub_at >= sum(split[:g]), out_recv[g], result)
    out[...] = result[0:targets, 0:local_m]

    @pl.when(active)
    def _():
        each_group(lambda g: pl.when(g != g_me)(lambda: out_copy(g, g_me).wait_send()))


def solution(mesh):
    groups, haps = mesh.shape["grp"], mesh.shape["hap"]

    def local(alleles, observed, map_steps, start_weights, end_weights):
        local_m, local_w = alleles.shape
        targets, total_haps = start_weights.shape
        words = local_w * haps
        bits_word = total_haps // words
        reps = LANE * SUB // words
        vecs = bits_word // reps
        pack = LANE // local_w
        slots = pack * -(-local_m // pack)
        size = block_size(local_m)
        blocks = groups * (local_m // size)
        split = split_targets(targets, groups * slots * total_haps * 4)
        each, teams = max(split), len(split)
        assert targets < SUB and teams <= groups and slots % SUB == 0
        dims = (groups, haps, local_m, targets, words, bits_word)
        f32, i32 = jnp.float32, jnp.int32
        dma = pltpu.SemaphoreType.DMA
        tile = (SUB, LANE)
        out = pl.pallas_call(
            functools.partial(kernel, dims),
            out_shape=pltpu.VMEM((targets, local_m), f32),
            in_specs=[pl.BlockSpec(memory_space=pltpu.HBM)] * 5,
            out_specs=pl.BlockSpec(memory_space=pltpu.VMEM),
            scratch_shapes=[
                pltpu.VMEM((local_m, local_w), i32),
                pltpu.VMEM((targets, local_m), i32),
                pltpu.SMEM((local_m,), i32),
                pltpu.VMEM((slots + SUB, LANE), i32),
                pltpu.VMEM(tile, i32),
                pltpu.VMEM(tile, i32),
                pltpu.VMEM((groups, haps * SUB, LANE), i32),
                pltpu.VMEM((groups, *tile), i32),
                pltpu.VMEM((groups * slots, *tile), i32),
                pltpu.VMEM((2 * each + 1, groups * slots + (size + 1) * SUB, LANE), f32),
                pltpu.VMEM((2, targets, total_haps), f32),
                pltpu.VMEM((vecs * SUB * targets, LANE), f32),
                pltpu.VMEM((each, vecs, *tile), f32),
                pltpu.VMEM((each, vecs, *tile), f32),
                pltpu.VMEM((each, groups * slots, vecs, *tile), f32),
                pltpu.VMEM((each, groups, size * (size + 1) // 2, *tile), f32),
                pltpu.VMEM((each, groups * slots, vecs, *tile), f32),
                pltpu.VMEM((each, blocks, vecs, *tile), f32),
                pltpu.VMEM((each, local_m, vecs, *tile), f32),
                pltpu.VMEM((each, groups * slots * SUB, LANE), f32),
                pltpu.VMEM((each, groups * slots * SUB, LANE), f32),
                pltpu.VMEM((groups, *tile), f32),
                pltpu.VMEM((teams, *tile), f32),
                dma((5,)), dma((teams, haps)), dma((groups, haps)), dma((teams,)), dma((groups,)),
                dma((groups,)), dma((teams,)),
            ],
            compiler_params=pltpu.CompilerParams(
                collective_id=0, has_side_effects=True, vmem_limit_bytes=60 * 1024 * 1024),
        )(alleles, observed.T, map_steps, start_weights, end_weights)
        return out.T

    in_specs = (P("grp", "hap"), P("grp", "hap"), P("grp"), P("hap", None), P("hap", None))
    return jax.shard_map(local, mesh=mesh, in_specs=in_specs, out_specs=P("grp", "hap"), check_vma=False)
```

```python
import functools
import jax
import jax.numpy as jnp
from jax import lax
from jax.experimental import pallas as pl
from jax.experimental.pallas import tpu as pltpu
from jax.sharding import PartitionSpec as P

error_rate = 0.01
map_unit = 100000.0
SUB, LANE = 8, 128
MESH = pl.DeviceIdType.MESH


def total(parts):
    parts = list(parts)
    while len(parts) > 1:
        parts = [a + b for a, b in zip(parts[::2], parts[1::2])] + parts[len(parts) // 2 * 2:]
    return parts[0]


def block_size(local_m):
    return next(n for n in (5, 4, 3, 2, 1) if local_m % n == 0)


def split_targets(targets, state_bytes):
    if targets > 1 and 2 * (targets - 1) * state_bytes <= 40 * 1024 * 1024:
        return targets // 2, targets - targets // 2
    return (1,) * targets


def kernel(dims, alleles, observed, steps, starts, ends, out,
           own_alleles, own_observed, own_steps, tmp, block, meta, recv, metas, bits, table, weights, staged,
           state_a, state_b, emit, runs, kept, kept_low, waiting, numer, denom, dos, out_recv,
           load_sem, send_sem, recv_sem, meta_send, meta_recv, out_send, out_recv_sem):
    groups, haps, local_m, targets, words, bits_word = dims
    total_haps = words * bits_word
    local_w = words // haps
    span = words // SUB
    reps = LANE // span
    vecs = bits_word // reps
    pack = LANE // local_w
    rows = -(-local_m // pack)
    slots = pack * rows
    share = haps // SUB
    size = block_size(local_m)
    blocks = local_m // size
    end_row = groups * slots
    split = split_targets(targets, groups * slots * total_haps * 4)
    teams = len(split)
    far = groups - 1
    g_me, h_me = lax.axis_index("grp"), lax.axis_index("hap")
    active = g_me < teams

    sources = [
        (alleles, own_alleles), (observed, own_observed), (steps, own_steps), (starts, weights.at[0]), (ends, weights.at[1])]
    loads = [pltpu.make_async_copy(source, target, load_sem.at[n]) for n, (source, target) in enumerate(sources)]
    for load in loads[:3]:
        load.start()

    def each_hap(act, first=0):
        if haps <= 8:
            for d in range(first, haps):
                act(lax.rem(h_me + d, haps))
        else:
            pl.loop(first, haps)(lambda d: act(lax.rem(h_me + d, haps)))

    def each_group(act):
        if groups <= 4:
            for g in range(groups):
                act(g)
        else:
            pl.loop(0, groups)(act)

    def not_me(g, h, act):
        pl.when((g != g_me) | (h != h_me))(act)

    barrier = pltpu.get_barrier_semaphore()

    def greet(g, h):
        pl.semaphore_signal(barrier, inc=1, device_id=(g, h), device_id_type=MESH)

    @pl.when(active)
    def _():
        each_group(lambda g: each_hap(lambda h: not_me(g, h, lambda: greet(g, h))))
        for load in loads[3:]:
            load.start()

    lane = lax.broadcasted_iota(jnp.int32, (SUB, LANE), 1)
    sub_at = lax.broadcasted_iota(jnp.int32, (SUB, LANE), 0)
    tmp[...] = jnp.zeros_like(tmp)
    for load in loads[:3]:
        load.wait()
    tmp[0:local_m, 0:local_w] = own_alleles[...]
    dense = tmp[0:SUB, :]
    for p in range(1, pack):
        dense = jnp.where(lane // local_w == p, pltpu.roll(tmp[p * rows:p * rows + SUB, :], p * local_w, 1), dense)
    block[...] = dense
    recv[g_me, pl.ds(pl.multiple_of(h_me * SUB, SUB), SUB), :] = dense
    tmp[0:targets, 0:local_m] = own_observed[...]
    columns = tmp[0:SUB, :]
    for i in range(local_m):
        columns = jnp.where((sub_at == targets) & (lane == i), own_steps[i], columns)
    meta[...] = columns
    metas[g_me] = columns

    def block_copy(g, h, from_g, from_h):
        return pltpu.make_async_remote_copy(
            src_ref=block, dst_ref=recv.at[from_g, pl.ds(pl.multiple_of(from_h * SUB, SUB), SUB), :],
            send_sem=send_sem.at[g, h], recv_sem=recv_sem.at[from_g, from_h],
            device_id=(g, h), device_id_type=MESH)

    def meta_copy(g, from_g):
        return pltpu.make_async_remote_copy(
            src_ref=meta, dst_ref=metas.at[from_g], send_sem=meta_send.at[g], recv_sem=meta_recv.at[from_g],
            device_id=(g, h_me), device_id_type=MESH)

    def each_send(act):
        for g in reversed(range(teams)):
            pl.when(g != g_me)(lambda: act(meta_copy(g, g_me)))
            each_hap(lambda h: not_me(g, h, lambda: act(block_copy(g, h, g_me, h_me))))

    pl.semaphore_wait(barrier, teams * haps - jnp.where(active, 1, 0))
    each_send(lambda copy: copy.start())

    def out_copy(g, from_g):
        return pltpu.make_async_remote_copy(
            src_ref=dos.at[g], dst_ref=out_recv.at[from_g], send_sem=out_send.at[g],
            recv_sem=out_recv_sem.at[from_g], device_id=(g, h_me), device_id_type=MESH)

    def run(first, each):
        def add_up(value):
            for shift in (4, 2, 1):
                value = value + pltpu.roll(value, shift, 0)
            return jnp.broadcast_to(jnp.sum(value, axis=1, keepdims=True), (SUB, LANE))

        def arrange(which, state):
            for r in range(vecs):
                for s in range(SUB):
                    at = s * vecs + r
                    staged[at * targets:(at + 1) * targets, :] = weights[which, :, at * LANE:(at + 1) * LANE]
            sums = [None] * each
            for q in range(vecs):
                spot = bits_word * (lane % span) + reps * q + lane // span
                chosen, within = spot // LANE, spot % LANE
                value = [jnp.zeros((SUB, LANE), jnp.float32)] * each
                for r in range(vecs):
                    here = chosen == r
                    for t in range(each):
                        source = staged[pl.ds(r * targets + first + t, SUB, stride=vecs * targets), :]
                        moved = jnp.take_along_axis(source, within, axis=1, mode="promise_in_bounds")
                        value[t] = jnp.where(here, moved, value[t])
                for t in range(each):
                    state[t, q] = value[t]
                    sums[t] = value[t] if q == 0 else sums[t] + value[t]
            return tuple(1.0 / add_up(sums[t]) for t in range(each))

        def meta_arrived(g):
            pl.when(g != g_me)(lambda: meta_copy(g_me, g).wait_recv())

        def arrived(g):
            each_hap(lambda h: not_me(g, h, lambda: block_copy(g_me, h_me, g, h).wait_recv()))

        def read_meta(g):
            same = lax.broadcasted_iota(jnp.int32, (slots, LANE), 0) == lax.broadcasted_iota(jnp.int32, (slots, LANE), 1)

            def turned(at):
                values = jnp.broadcast_to(metas[g, pl.ds(at, 1), :].astype(jnp.float32), (slots, LANE))
                summed = jnp.sum(jnp.where(same, values, 0.0), axis=1, keepdims=True)
                return jnp.broadcast_to(summed, (slots, LANE))

            at = pl.ds(pl.multiple_of(g * slots, SUB), slots)
            for t in range(each):
                seen = turned(first + t)
                table[2 * t, at, :] = jnp.where(seen == 2.0, 1.0, jnp.where(seen == 1.0, 1.0 - error_rate, error_rate))
                table[2 * t + 1, at, :] = jnp.where(seen == 2.0, 1.0, jnp.where(seen == 0.0, 1.0 - error_rate, error_rate))
            rate = 1.0 - jnp.exp(-turned(targets) / map_unit)
            table[2 * each, at, :] = (rate / total_haps) / (1.0 - rate)

        def expand(g):
            for r in range(rows):
                parts = [recv[g, pl.ds(j * SUB + r, SUB, stride=SUB * share), :] for j in range(share)]
                for p in range(pack):
                    n = p * rows + r
                    if n >= local_m:
                        continue
                    value = jnp.zeros((SUB, LANE), jnp.int32)
                    for e in range(reps):
                        for j in range(share):
                            begin = e * span + j * local_w
                            shift = (begin - p * local_w) % LANE
                            piece = parts[j] if shift == 0 else pltpu.roll(parts[j], shift, 1)
                            piece = piece if e == 0 else jnp.right_shift(piece, e)
                            value = jnp.where((lane >= begin) & (lane < begin + local_w), piece, value)
                    bits[g * slots + n] = value

        def row(kind, slot):
            return jnp.broadcast_to(table[kind, pl.ds(slot, 1), :], (SUB, LANE))

        def masked(words_in, q):
            return jnp.bitwise_and(words_in, 1 << (reps * q)) != 0

        pairs = [(j, i) for j in range(size) for i in range(j, size)]
        team = range(each)

        def prepare(g, n):
            at = g * slots + n * size
            words_in = [bits[at + i] for i in range(size)]
            tops = [[(row(2 * t, at + i), row(2 * t + 1, at + i)) for i in range(size)] for t in team]
            for q in range(vecs):
                for i in range(size):
                    mask = masked(words_in[i], q)
                    for t in team:
                        emit[t, at + i, q] = jnp.where(mask, *tops[t][i])
                        kept[t, at + i, q] = jnp.where(mask, tops[t][i][0], 0.0)

        inner = min(size, 4)
        used = sum(1 << (reps * q) for q in range(vecs))

        def count_patterns(g):
            counts = [jnp.zeros((SUB, LANE), jnp.float32)] * (1 << (size - inner))
            for n in range(blocks):
                sets = [jnp.full((SUB, LANE), used, jnp.int32)]
                for i in range(size):
                    word = bits[g * slots + n * size + i]
                    other = jnp.bitwise_not(word)
                    sets = [jnp.bitwise_and(x, other) for x in sets] + [jnp.bitwise_and(x, word) for x in sets]
                sets += [jnp.zeros((SUB, LANE), jnp.int32)] * (LANE // SUB - len(sets))
                held = jnp.concatenate([lax.population_count(x).astype(jnp.float32) for x in sets], axis=0)
                found = lax.dot_general(
                    jnp.ones((SUB, LANE), jnp.bfloat16), held.astype(jnp.bfloat16), (((1,), (1,)), ((), ())),
                    preferred_element_type=jnp.float32)
                counts = [jnp.where(sub_at == n, found[:, k * LANE:(k + 1) * LANE], c) for k, c in enumerate(counts)]
            return counts

        def make_spans(g):
            counts = count_patterns(g)
            pattern = lane // SUB
            for t in team:
                def rows_of(kind, i):
                    return table[kind, pl.ds(g * slots + i, SUB, stride=size), :]

                e = [
                    jnp.where(jnp.bitwise_and(jnp.right_shift(pattern, i), 1) != 0, rows_of(2 * t, i), rows_of(2 * t + 1, i))
                    for i in range(inner)
                ]
                whole = total(counts)
                if size > inner:
                    last = counts[0] * rows_of(2 * t + 1, inner) + counts[1] * rows_of(2 * t, inner)
                for j in range(size):
                    run = None
                    for i in range(j, size):
                        if i < inner:
                            run = e[i] if run is None else run * e[i]
                            value = whole * run
                        else:
                            value = last if run is None else last * run
                        summed = jnp.broadcast_to(jnp.sum(value, axis=1, keepdims=True), (SUB, LANE))
                        runs[t, g, pairs.index((j, i))] = summed

        def ahead(t, state, g, n, order):
            at = g * slots + n * size
            sums = [None] * size
            for q in range(vecs):
                value = state[t, q]
                for i in order:
                    value = value * emit[t, at + i, q]
                    sums[i] = value if q == 0 else sums[i] + value
            return [add_up(value) for value in sums]

        def solve(t, sums, scale, g, n, order, after):
            at = g * slots + n * size
            span_of = {
                pair: jnp.broadcast_to(runs[t, g, k, pl.ds(n, 1), :], (SUB, LANE)) for k, pair in enumerate(pairs)}
            adds = {}
            last = None
            for i in order:
                slot = at + i
                if after:
                    slot = slot + 1
                    if i == size - 1:
                        ahead = jnp.where(g + 1 < groups, (g + 1) * slots, end_row)
                        slot = jnp.where(n * size + size == local_m, ahead, slot)
                adds[i] = row(2 * each, slot) if last is None else row(2 * each, slot) * last
                last = sums[i] * scale
                for j in adds:
                    last = last + adds[j] * span_of[min(i, j), max(i, j)]
            return adds, 1.0 / last

        up, down = list(range(size)), list(range(size))[::-1]

        def step_a(g, n, scale):
            at = g * slots + n * size
            sums = [ahead(t, state_a, g, n, up) for t in team]
            solved = [solve(t, sums[t], scale[t], g, n, up, False) for t in team]
            for t in team:
                for q in range(vecs):
                    value = state_a[t, q] * scale[t]
                    for i in up:
                        moved = value + solved[t][0][i]
                        kept[t, at + i, q] = kept[t, at + i, q] * moved
                        value = emit[t, at + i, q] * moved
                    kept_low[t, g * blocks + n, q] = value
                    state_a[t, q] = value
            return tuple(solved[t][1] for t in team)

        def put_sums(t, g, n, tops, low):
            for i in range(size):
                at = pl.ds(pl.multiple_of((g * slots + n * size + i) * SUB, SUB), SUB)
                numer[t, at, :] = tops[i]
                denom[t, at, :] = low

        def step_b(t, g, n, scale, sums, score):
            at = g * slots + n * size
            adds, after = solve(t, sums, scale, g, n, down, True)
            tops, low = [None] * size, None
            for q in range(vecs):
                value = state_b[t, q] * scale
                for i in down:
                    value = value + adds[i]
                    if not score:
                        waiting[t, n * size + i, q] = value
                    else:
                        part = kept[t, at + i, q] * value
                        tops[i] = part if q == 0 else tops[i] + part
                        if i == size - 1:
                            part = kept_low[t, g * blocks + n, q] * value
                            low = part if q == 0 else low + part
                    value = emit[t, at + i, q] * value
                state_b[t, q] = value
            if score:
                put_sums(t, g, n, tops, low)
            return after

        def score_waiting(g, n):
            at = g * slots + n * size
            end = n * size + size - 1
            for t in team:
                tops, low = [None] * size, None
                for q in range(vecs):
                    for i in range(size):
                        part = kept[t, at + i, q] * waiting[t, n * size + i, q]
                        tops[i] = part if q == 0 else tops[i] + part
                    part = kept_low[t, g * blocks + n, q] * waiting[t, end, q]
                    low = part if q == 0 else low + part
                put_sums(t, g, n, tops, low)

        row_at = lax.broadcasted_iota(jnp.int32, (slots, LANE), 0)
        own_lane = (lax.broadcasted_iota(jnp.int32, (slots, LANE), 1) == row_at) & (row_at < local_m)

        def finish(g):
            result = jnp.zeros((SUB, LANE), jnp.float32)
            for t in team:
                def gathered(sums):
                    parts = [sums[t, pl.ds(g * slots * SUB + k, slots, stride=SUB), :] for k in range(SUB)]
                    return jnp.sum(total(parts), axis=1, keepdims=True)

                value = jnp.broadcast_to(gathered(numer) / gathered(denom), (slots, LANE))
                value = jnp.sum(jnp.where(own_lane, value, 0.0), axis=0, keepdims=True)
                result = jnp.where(sub_at == first + t, jnp.broadcast_to(value, (SUB, LANE)), result)
            dos[g] = result
            pl.when(g != g_me)(lambda: out_copy(g, g_me).start())

        for load in loads[3:]:
            load.wait()
        scale_a = arrange(0, state_a)
        scale_b = arrange(1, state_b)
        table[2 * each, end_row:end_row + SUB, :] = jnp.zeros((SUB, LANE), jnp.float32)

        def first_pass(g, scale):
            meta_arrived(g)
            arrived(g)
            expand(g)
            read_meta(g)
            make_spans(g)
            for n in range(blocks):
                prepare(g, n)
                scale = step_a(g, n, scale)
            return scale

        scale_a = lax.fori_loop(0, far, first_pass, scale_a)
        meta_arrived(far)
        read_meta(far)
        arrived(far)
        expand(far)
        make_spans(far)
        ready = set()
        for n in range(blocks):
            m = blocks - 1 - n
            for k in sorted({n, m} - ready):
                prepare(far, k)
            ready |= {n, m}
            scale_a = step_a(far, n, scale_a)
            sums = [ahead(t, state_b, far, m, down) for t in team]
            scale_b = tuple(step_b(t, far, m, scale_b[t], sums[t], False) for t in team)

        sums = ahead(0, state_b, far - 1, blocks - 1, down)
        for n in range(blocks):
            score_waiting(far, n)

        def second_pass(k, carry):
            g = far - 1 - k
            scale, sums = list(carry[0]), list(carry[1])
            for n in reversed(range(blocks)):
                scale[0] = step_b(0, g, n, scale[0], sums, True)
                if n:
                    sums = ahead(0, state_b, g, n - 1, down)
                elif groups > 4 or g > 0:
                    sums = ahead(0, state_b, jnp.maximum(g - 1, 0) if groups > 4 else g - 1, blocks - 1, down)
                for t in range(1, each):
                    scale[t] = step_b(t, g, n, scale[t], ahead(t, state_b, g, n, down), True)
                if n + 1 == blocks:
                    finish(g + 1)
            return tuple(scale), tuple(sums)

        carry = scale_b, tuple(sums)
        if groups <= 4:
            for k in range(far):
                carry = second_pass(k, carry)
        else:
            lax.fori_loop(0, far, second_pass, carry)
        finish(0)
        out_recv[g_me] = dos[g_me]

    if len(set(split)) == 1:
        pl.when(active)(lambda: run(g_me * split[0], split[0]))
    else:
        for g in range(teams):
            pl.when(g_me == g)(functools.partial(run, sum(split[:g]), split[g]))

    each_send(lambda copy: copy.wait_send())
    for g in range(teams):
        pl.when(g != g_me)(lambda: out_copy(g_me, g).wait_recv())
    result = out_recv[0]
    for g in range(1, teams):
        result = jnp.where(sub_at >= sum(split[:g]), out_recv[g], result)
    out[...] = result[0:targets, 0:local_m]

    @pl.when(active)
    def _():
        each_group(lambda g: pl.when(g != g_me)(lambda: out_copy(g, g_me).wait_send()))


def solution(mesh):
    groups, haps = mesh.shape["grp"], mesh.shape["hap"]

    def local(alleles, observed, map_steps, start_weights, end_weights):
        local_m, local_w = alleles.shape
        targets, total_haps = start_weights.shape
        words = local_w * haps
        bits_word = total_haps // words
        reps = LANE * SUB // words
        vecs = bits_word // reps
        pack = LANE // local_w
        slots = pack * -(-local_m // pack)
        size = block_size(local_m)
        blocks = groups * (local_m // size)
        split = split_targets(targets, groups * slots * total_haps * 4)
        each, teams = max(split), len(split)
        assert targets < SUB and teams <= groups and slots % SUB == 0
        dims = (groups, haps, local_m, targets, words, bits_word)
        f32, i32 = jnp.float32, jnp.int32
        dma = pltpu.SemaphoreType.DMA
        tile = (SUB, LANE)
        out = pl.pallas_call(
            functools.partial(kernel, dims),
            out_shape=pltpu.VMEM((targets, local_m), f32),
            in_specs=[pl.BlockSpec(memory_space=pltpu.HBM)] * 5,
            out_specs=pl.BlockSpec(memory_space=pltpu.VMEM),
            scratch_shapes=[
                pltpu.VMEM((local_m, local_w), i32),
                pltpu.VMEM((targets, local_m), i32),
                pltpu.SMEM((local_m,), i32),
                pltpu.VMEM((slots + SUB, LANE), i32),
                pltpu.VMEM(tile, i32),
                pltpu.VMEM(tile, i32),
                pltpu.VMEM((groups, haps * SUB, LANE), i32),
                pltpu.VMEM((groups, *tile), i32),
                pltpu.VMEM((groups * slots, *tile), i32),
                pltpu.VMEM((2 * each + 1, groups * slots + (size + 1) * SUB, LANE), f32),
                pltpu.VMEM((2, targets, total_haps), f32),
                pltpu.VMEM((vecs * SUB * targets, LANE), f32),
                pltpu.VMEM((each, vecs, *tile), f32),
                pltpu.VMEM((each, vecs, *tile), f32),
                pltpu.VMEM((each, groups * slots, vecs, *tile), f32),
                pltpu.VMEM((each, groups, size * (size + 1) // 2, *tile), f32),
                pltpu.VMEM((each, groups * slots, vecs, *tile), f32),
                pltpu.VMEM((each, blocks, vecs, *tile), f32),
                pltpu.VMEM((each, local_m, vecs, *tile), f32),
                pltpu.VMEM((each, groups * slots * SUB, LANE), f32),
                pltpu.VMEM((each, groups * slots * SUB, LANE), f32),
                pltpu.VMEM((groups, *tile), f32),
                pltpu.VMEM((teams, *tile), f32),
                dma((5,)), dma((teams, haps)), dma((groups, haps)), dma((teams,)), dma((groups,)),
                dma((groups,)), dma((teams,)),
            ],
            compiler_params=pltpu.CompilerParams(
                collective_id=0, has_side_effects=True, vmem_limit_bytes=60 * 1024 * 1024),
        )(alleles, observed.T, map_steps, start_weights, end_weights)
        return out.T

    in_specs = (P("grp", "hap"), P("grp", "hap"), P("grp"), P("hap", None), P("hap", None))
    return jax.shard_map(local, mesh=mesh, in_specs=in_specs, out_specs=P("grp", "hap"), check_vma=False)
```

```python
import functools
import jax
import jax.numpy as jnp
from jax import lax
from jax.experimental import pallas as pl
from jax.experimental.pallas import tpu as pltpu
from jax.sharding import PartitionSpec as P

error_rate = 0.01
map_unit = 100000.0
SUB, LANE = 8, 128
MESH = pl.DeviceIdType.MESH


def total(parts):
    parts = list(parts)
    while len(parts) > 1:
        parts = [a + b for a, b in zip(parts[::2], parts[1::2])] + parts[len(parts) // 2 * 2:]
    return parts[0]


def block_size(local_m):
    return next(n for n in (5, 4, 3, 2, 1) if local_m % n == 0)


def split_targets(targets, state_bytes):
    if targets > 1 and 2 * (targets - 1) * state_bytes <= 40 * 1024 * 1024:
        return targets // 2, targets - targets // 2
    return (1,) * targets


def kernel(dims, alleles, observed, steps, starts, ends, out,
           own_alleles, own_observed, own_steps, tmp, block, meta, recv, metas, bits, table, weights, staged,
           state_a, state_b, emit, runs, kept, kept_low, waiting, numer, denom, dos, out_recv,
           load_sem, send_sem, recv_sem, meta_send, meta_recv, out_send, out_recv_sem):
    groups, haps, local_m, targets, words, bits_word = dims
    total_haps = words * bits_word
    local_w = words // haps
    span = words // SUB
    reps = LANE // span
    vecs = bits_word // reps
    pack = LANE // local_w
    rows = -(-local_m // pack)
    slots = pack * rows
    share = haps // SUB
    size = block_size(local_m)
    blocks = local_m // size
    end_row = groups * slots
    split = split_targets(targets, groups * slots * total_haps * 4)
    teams = len(split)
    far = groups - 1
    g_me, h_me = lax.axis_index("grp"), lax.axis_index("hap")
    active = g_me < teams

    sources = [
        (alleles, own_alleles), (observed, own_observed), (steps, own_steps), (starts, weights.at[0]), (ends, weights.at[1])]
    loads = [pltpu.make_async_copy(source, target, load_sem.at[n]) for n, (source, target) in enumerate(sources)]
    for load in loads[:3]:
        load.start()

    def each_hap(act, first=0):
        if haps <= 8:
            for d in range(first, haps):
                act(lax.rem(h_me + d, haps))
        else:
            pl.loop(first, haps)(lambda d: act(lax.rem(h_me + d, haps)))

    def each_group(act):
        if groups <= 4:
            for g in range(groups):
                act(g)
        else:
            pl.loop(0, groups)(act)

    def not_me(g, h, act):
        pl.when((g != g_me) | (h != h_me))(act)

    barrier = pltpu.get_barrier_semaphore()

    def greet(g, h):
        pl.semaphore_signal(barrier, inc=1, device_id=(g, h), device_id_type=MESH)

    @pl.when(active)
    def _():
        each_group(lambda g: each_hap(lambda h: not_me(g, h, lambda: greet(g, h))))
        for load in loads[3:]:
            load.start()

    lane = lax.broadcasted_iota(jnp.int32, (SUB, LANE), 1)
    sub_at = lax.broadcasted_iota(jnp.int32, (SUB, LANE), 0)
    tmp[...] = jnp.zeros_like(tmp)
    for load in loads[:3]:
        load.wait()
    tmp[0:local_m, 0:local_w] = own_alleles[...]
    dense = tmp[0:SUB, :]
    for p in range(1, pack):
        dense = jnp.where(lane // local_w == p, pltpu.roll(tmp[p * rows:p * rows + SUB, :], p * local_w, 1), dense)
    block[...] = dense
    recv[g_me, pl.ds(pl.multiple_of(h_me * SUB, SUB), SUB), :] = dense
    tmp[0:targets, 0:local_m] = own_observed[...]
    columns = tmp[0:SUB, :]
    for i in range(local_m):
        columns = jnp.where((sub_at == targets) & (lane == i), own_steps[i], columns)
    meta[...] = columns
    metas[g_me] = columns

    def block_copy(g, h, from_g, from_h):
        return pltpu.make_async_remote_copy(
            src_ref=block, dst_ref=recv.at[from_g, pl.ds(pl.multiple_of(from_h * SUB, SUB), SUB), :],
            send_sem=send_sem.at[g, h], recv_sem=recv_sem.at[from_g, from_h],
            device_id=(g, h), device_id_type=MESH)

    def meta_copy(g, from_g):
        return pltpu.make_async_remote_copy(
            src_ref=meta, dst_ref=metas.at[from_g], send_sem=meta_send.at[g], recv_sem=meta_recv.at[from_g],
            device_id=(g, h_me), device_id_type=MESH)

    def each_send(act):
        for g in reversed(range(teams)):
            pl.when(g != g_me)(lambda: act(meta_copy(g, g_me)))
            each_hap(lambda h: not_me(g, h, lambda: act(block_copy(g, h, g_me, h_me))))

    pl.semaphore_wait(barrier, teams * haps - jnp.where(active, 1, 0))
    each_send(lambda copy: copy.start())

    def out_copy(g, from_g):
        return pltpu.make_async_remote_copy(
            src_ref=dos.at[g], dst_ref=out_recv.at[from_g], send_sem=out_send.at[g],
            recv_sem=out_recv_sem.at[from_g], device_id=(g, h_me), device_id_type=MESH)

    def run(first, each):
        def add_up(value):
            for shift in (4, 2, 1):
                value = value + pltpu.roll(value, shift, 0)
            return jnp.broadcast_to(jnp.sum(value, axis=1, keepdims=True), (SUB, LANE))

        def arrange(which, state):
            for r in range(vecs):
                for s in range(SUB):
                    at = s * vecs + r
                    staged[at * targets:(at + 1) * targets, :] = weights[which, :, at * LANE:(at + 1) * LANE]
            sums = [None] * each
            for q in range(vecs):
                spot = bits_word * (lane % span) + reps * q + lane // span
                chosen, within = spot // LANE, spot % LANE
                value = [jnp.zeros((SUB, LANE), jnp.float32)] * each
                for r in range(vecs):
                    here = chosen == r
                    for t in range(each):
                        source = staged[pl.ds(r * targets + first + t, SUB, stride=vecs * targets), :]
                        moved = jnp.take_along_axis(source, within, axis=1, mode="promise_in_bounds")
                        value[t] = jnp.where(here, moved, value[t])
                for t in range(each):
                    state[t, q] = value[t]
                    sums[t] = value[t] if q == 0 else sums[t] + value[t]
            return tuple(1.0 / add_up(sums[t]) for t in range(each))

        def meta_arrived(g):
            pl.when(g != g_me)(lambda: meta_copy(g_me, g).wait_recv())

        def arrived(g):
            each_hap(lambda h: not_me(g, h, lambda: block_copy(g_me, h_me, g, h).wait_recv()))

        def read_meta(g):
            same = lax.broadcasted_iota(jnp.int32, (slots, LANE), 0) == lax.broadcasted_iota(jnp.int32, (slots, LANE), 1)

            def turned(at):
                values = jnp.broadcast_to(metas[g, pl.ds(at, 1), :].astype(jnp.float32), (slots, LANE))
                summed = jnp.sum(jnp.where(same, values, 0.0), axis=1, keepdims=True)
                return jnp.broadcast_to(summed, (slots, LANE))

            at = pl.ds(pl.multiple_of(g * slots, SUB), slots)
            for t in range(each):
                seen = turned(first + t)
                table[2 * t, at, :] = jnp.where(seen == 2.0, 1.0, jnp.where(seen == 1.0, 1.0 - error_rate, error_rate))
                table[2 * t + 1, at, :] = jnp.where(seen == 2.0, 1.0, jnp.where(seen == 0.0, 1.0 - error_rate, error_rate))
            rate = 1.0 - jnp.exp(-turned(targets) / map_unit)
            table[2 * each, at, :] = (rate / total_haps) / (1.0 - rate)

        def expand(g):
            for r in range(rows):
                parts = [recv[g, pl.ds(j * SUB + r, SUB, stride=SUB * share), :] for j in range(share)]
                for p in range(pack):
                    n = p * rows + r
                    if n >= local_m:
                        continue
                    value = jnp.zeros((SUB, LANE), jnp.int32)
                    for e in range(reps):
                        for j in range(share):
                            begin = e * span + j * local_w
                            shift = (begin - p * local_w) % LANE
                            piece = parts[j] if shift == 0 else pltpu.roll(parts[j], shift, 1)
                            piece = piece if e == 0 else jnp.right_shift(piece, e)
                            value = jnp.where((lane >= begin) & (lane < begin + local_w), piece, value)
                    bits[g * slots + n] = value

        def row(kind, slot):
            return jnp.broadcast_to(table[kind, pl.ds(slot, 1), :], (SUB, LANE))

        def masked(words_in, q):
            return jnp.bitwise_and(words_in, 1 << (reps * q)) != 0

        pairs = [(j, i) for j in range(size) for i in range(j, size)]
        team = range(each)

        def prepare(g, n):
            at = g * slots + n * size
            words_in = [bits[at + i] for i in range(size)]
            tops = [[(row(2 * t, at + i), row(2 * t + 1, at + i)) for i in range(size)] for t in team]
            for q in range(vecs):
                for i in range(size):
                    mask = masked(words_in[i], q)
                    for t in team:
                        emit[t, at + i, q] = jnp.where(mask, *tops[t][i])
                        kept[t, at + i, q] = jnp.where(mask, tops[t][i][0], 0.0)

        inner = min(size, 4)
        used = sum(1 << (reps * q) for q in range(vecs))

        def count_patterns(g):
            counts = [jnp.zeros((SUB, LANE), jnp.float32)] * (1 << (size - inner))
            for n in range(blocks):
                sets = [jnp.full((SUB, LANE), used, jnp.int32)]
                for i in range(size):
                    word = bits[g * slots + n * size + i]
                    other = jnp.bitwise_not(word)
                    sets = [jnp.bitwise_and(x, other) for x in sets] + [jnp.bitwise_and(x, word) for x in sets]
                sets += [jnp.zeros((SUB, LANE), jnp.int32)] * (LANE // SUB - len(sets))
                held = jnp.concatenate([lax.population_count(x).astype(jnp.float32) for x in sets], axis=0)
                found = lax.dot_general(
                    jnp.ones((SUB, LANE), jnp.bfloat16), held.astype(jnp.bfloat16), (((1,), (1,)), ((), ())),
                    preferred_element_type=jnp.float32)
                counts = [jnp.where(sub_at == n, found[:, k * LANE:(k + 1) * LANE], c) for k, c in enumerate(counts)]
            return counts

        def make_spans(g):
            counts = count_patterns(g)
            pattern = lane // SUB
            for t in team:
                def rows_of(kind, i):
                    return table[kind, pl.ds(g * slots + i, SUB, stride=size), :]

                e = [
                    jnp.where(jnp.bitwise_and(jnp.right_shift(pattern, i), 1) != 0, rows_of(2 * t, i), rows_of(2 * t + 1, i))
                    for i in range(inner)
                ]
                whole = total(counts)
                if size > inner:
                    last = counts[0] * rows_of(2 * t + 1, inner) + counts[1] * rows_of(2 * t, inner)
                for j in range(size):
                    run = None
                    for i in range(j, size):
                        if i < inner:
                            run = e[i] if run is None else run * e[i]
                            value = whole * run
                        else:
                            value = last if run is None else last * run
                        summed = jnp.broadcast_to(jnp.sum(value, axis=1, keepdims=True), (SUB, LANE))
                        runs[t, g, pairs.index((j, i))] = summed

        def ahead(t, state, g, n, order):
            at = g * slots + n * size
            sums = [None] * size
            for q in range(vecs):
                value = state[t, q]
                for i in order:
                    value = value * emit[t, at + i, q]
                    sums[i] = value if q == 0 else sums[i] + value
            return [add_up(value) for value in sums]

        def solve(t, sums, scale, g, n, order, after):
            at = g * slots + n * size
            span_of = {
                pair: jnp.broadcast_to(runs[t, g, k, pl.ds(n, 1), :], (SUB, LANE)) for k, pair in enumerate(pairs)}
            adds = {}
            last = None
            for i in order:
                slot = at + i
                if after:
                    slot = slot + 1
                    if i == size - 1:
                        ahead = jnp.where(g + 1 < groups, (g + 1) * slots, end_row)
                        slot = jnp.where(n * size + size == local_m, ahead, slot)
                adds[i] = row(2 * each, slot) if last is None else row(2 * each, slot) * last
                last = sums[i] * scale
                for j in adds:
                    last = last + adds[j] * span_of[min(i, j), max(i, j)]
            return adds, 1.0 / last

        up, down = list(range(size)), list(range(size))[::-1]

        def step_a(g, n, scale):
            at = g * slots + n * size
            sums = [ahead(t, state_a, g, n, up) for t in team]
            solved = [solve(t, sums[t], scale[t], g, n, up, False) for t in team]
            for t in team:
                for q in range(vecs):
                    value = state_a[t, q] * scale[t]
                    for i in up:
                        moved = value + solved[t][0][i]
                        kept[t, at + i, q] = kept[t, at + i, q] * moved
                        value = emit[t, at + i, q] * moved
                    kept_low[t, g * blocks + n, q] = value
                    state_a[t, q] = value
            return tuple(solved[t][1] for t in team)

        def put_sums(t, g, n, tops, low):
            for i in range(size):
                at = pl.ds(pl.multiple_of((g * slots + n * size + i) * SUB, SUB), SUB)
                numer[t, at, :] = tops[i]
                denom[t, at, :] = low

        def step_b(t, g, n, scale, sums, score):
            at = g * slots + n * size
            adds, after = solve(t, sums, scale, g, n, down, True)
            tops, low = [None] * size, None
            for q in range(vecs):
                value = state_b[t, q] * scale
                for i in down:
                    value = value + adds[i]
                    if not score:
                        waiting[t, n * size + i, q] = value
                    else:
                        part = kept[t, at + i, q] * value
                        tops[i] = part if q == 0 else tops[i] + part
                        if i == size - 1:
                            part = kept_low[t, g * blocks + n, q] * value
                            low = part if q == 0 else low + part
                    value = emit[t, at + i, q] * value
                state_b[t, q] = value
            if score:
                put_sums(t, g, n, tops, low)
            return after

        def score_waiting(g, n):
            at = g * slots + n * size
            end = n * size + size - 1
            for t in team:
                tops, low = [None] * size, None
                for q in range(vecs):
                    for i in range(size):
                        part = kept[t, at + i, q] * waiting[t, n * size + i, q]
                        tops[i] = part if q == 0 else tops[i] + part
                    part = kept_low[t, g * blocks + n, q] * waiting[t, end, q]
                    low = part if q == 0 else low + part
                put_sums(t, g, n, tops, low)

        row_at = lax.broadcasted_iota(jnp.int32, (slots, LANE), 0)
        own_lane = (lax.broadcasted_iota(jnp.int32, (slots, LANE), 1) == row_at) & (row_at < local_m)

        def finish(g):
            result = jnp.zeros((SUB, LANE), jnp.float32)
            for t in team:
                def gathered(sums):
                    parts = [sums[t, pl.ds(g * slots * SUB + k, slots, stride=SUB), :] for k in range(SUB)]
                    return jnp.sum(total(parts), axis=1, keepdims=True)

                value = jnp.broadcast_to(gathered(numer) / gathered(denom), (slots, LANE))
                value = jnp.sum(jnp.where(own_lane, value, 0.0), axis=0, keepdims=True)
                result = jnp.where(sub_at == first + t, jnp.broadcast_to(value, (SUB, LANE)), result)
            dos[g] = result
            pl.when(g != g_me)(lambda: out_copy(g, g_me).start())

        for load in loads[3:]:
            load.wait()
        scale_a = arrange(0, state_a)
        scale_b = arrange(1, state_b)
        table[2 * each, end_row:end_row + SUB, :] = jnp.zeros((SUB, LANE), jnp.float32)

        meta_arrived(0)
        read_meta(0)

        def first_pass(g, scale):
            arrived(g)
            meta_arrived(g + 1)
            expand(g)
            read_meta(g + 1)
            make_spans(g)
            for n in range(blocks):
                prepare(g, n)
                scale = step_a(g, n, scale)
            return scale

        scale_a = lax.fori_loop(0, far, first_pass, scale_a)
        arrived(far)
        expand(far)
        make_spans(far)
        ready = set()
        for n in range(blocks):
            m = blocks - 1 - n
            for k in sorted({n, m} - ready):
                prepare(far, k)
            ready |= {n, m}
            scale_a = step_a(far, n, scale_a)
            sums = [ahead(t, state_b, far, m, down) for t in team]
            scale_b = tuple(step_b(t, far, m, scale_b[t], sums[t], False) for t in team)

        sums = ahead(0, state_b, far - 1, blocks - 1, down)
        for n in range(blocks):
            score_waiting(far, n)

        def second_pass(k, carry):
            g = far - 1 - k
            scale, sums = list(carry[0]), list(carry[1])
            for n in reversed(range(blocks)):
                scale[0] = step_b(0, g, n, scale[0], sums, True)
                if n:
                    sums = ahead(0, state_b, g, n - 1, down)
                elif groups > 4 or g > 0:
                    sums = ahead(0, state_b, jnp.maximum(g - 1, 0) if groups > 4 else g - 1, blocks - 1, down)
                for t in range(1, each):
                    scale[t] = step_b(t, g, n, scale[t], ahead(t, state_b, g, n, down), True)
                if n + 1 == blocks:
                    finish(g + 1)
            return tuple(scale), tuple(sums)

        carry = scale_b, tuple(sums)
        if groups <= 4:
            for k in range(far):
                carry = second_pass(k, carry)
        else:
            lax.fori_loop(0, far, second_pass, carry)
        finish(0)
        out_recv[g_me] = dos[g_me]

    if len(set(split)) == 1:
        pl.when(active)(lambda: run(g_me * split[0], split[0]))
    else:
        for g in range(teams):
            pl.when(g_me == g)(functools.partial(run, sum(split[:g]), split[g]))

    each_send(lambda copy: copy.wait_send())
    for g in range(teams):
        pl.when(g != g_me)(lambda: out_copy(g_me, g).wait_recv())
    result = out_recv[0]
    for g in range(1, teams):
        result = jnp.where(sub_at >= sum(split[:g]), out_recv[g], result)
    out[...] = result[0:targets, 0:local_m]

    @pl.when(active)
    def _():
        each_group(lambda g: pl.when(g != g_me)(lambda: out_copy(g, g_me).wait_send()))


def solution(mesh):
    groups, haps = mesh.shape["grp"], mesh.shape["hap"]

    def local(alleles, observed, map_steps, start_weights, end_weights):
        local_m, local_w = alleles.shape
        targets, total_haps = start_weights.shape
        words = local_w * haps
        bits_word = total_haps // words
        reps = LANE * SUB // words
        vecs = bits_word // reps
        pack = LANE // local_w
        slots = pack * -(-local_m // pack)
        size = block_size(local_m)
        blocks = groups * (local_m // size)
        split = split_targets(targets, groups * slots * total_haps * 4)
        each, teams = max(split), len(split)
        assert targets < SUB and teams <= groups and slots % SUB == 0
        dims = (groups, haps, local_m, targets, words, bits_word)
        f32, i32 = jnp.float32, jnp.int32
        dma = pltpu.SemaphoreType.DMA
        tile = (SUB, LANE)
        out = pl.pallas_call(
            functools.partial(kernel, dims),
            out_shape=pltpu.VMEM((targets, local_m), f32),
            in_specs=[pl.BlockSpec(memory_space=pltpu.HBM)] * 5,
            out_specs=pl.BlockSpec(memory_space=pltpu.VMEM),
            scratch_shapes=[
                pltpu.VMEM((local_m, local_w), i32),
                pltpu.VMEM((targets, local_m), i32),
                pltpu.SMEM((local_m,), i32),
                pltpu.VMEM((slots + SUB, LANE), i32),
                pltpu.VMEM(tile, i32),
                pltpu.VMEM(tile, i32),
                pltpu.VMEM((groups, haps * SUB, LANE), i32),
                pltpu.VMEM((groups, *tile), i32),
                pltpu.VMEM((groups * slots, *tile), i32),
                pltpu.VMEM((2 * each + 1, groups * slots + (size + 1) * SUB, LANE), f32),
                pltpu.VMEM((2, targets, total_haps), f32),
                pltpu.VMEM((vecs * SUB * targets, LANE), f32),
                pltpu.VMEM((each, vecs, *tile), f32),
                pltpu.VMEM((each, vecs, *tile), f32),
                pltpu.VMEM((each, groups * slots, vecs, *tile), f32),
                pltpu.VMEM((each, groups, size * (size + 1) // 2, *tile), f32),
                pltpu.VMEM((each, groups * slots, vecs, *tile), f32),
                pltpu.VMEM((each, blocks, vecs, *tile), f32),
                pltpu.VMEM((each, local_m, vecs, *tile), f32),
                pltpu.VMEM((each, groups * slots * SUB, LANE), f32),
                pltpu.VMEM((each, groups * slots * SUB, LANE), f32),
                pltpu.VMEM((groups, *tile), f32),
                pltpu.VMEM((teams, *tile), f32),
                dma((5,)), dma((teams, haps)), dma((groups, haps)), dma((teams,)), dma((groups,)),
                dma((groups,)), dma((teams,)),
            ],
            compiler_params=pltpu.CompilerParams(
                collective_id=0, has_side_effects=True, vmem_limit_bytes=60 * 1024 * 1024),
        )(alleles, observed.T, map_steps, start_weights, end_weights)
        return out.T

    in_specs = (P("grp", "hap"), P("grp", "hap"), P("grp"), P("hap", None), P("hap", None))
    return jax.shard_map(local, mesh=mesh, in_specs=in_specs, out_specs=P("grp", "hap"), check_vma=False)
```
